256 devices in a mesh: branch: 64 (over z, x, core), col: 4 (over y).
Axes of the slice: x: 4, y: 4, z: 8, core: 2. Of those that a mesh axis runs over, the one named last changes fastest.
Arguments:
- vectors: bfloat16 [128, 524288], P('col', 'branch'), may hold values from -6 to 6
- basis: bfloat16 [2, 2048, 64, 256], P(None, 'branch'), may hold values from -0.375 to 0.375
- leaf_transfer: bfloat16 [2, 64, 131072], P(None, None, 'branch'), may hold values from -0.125 to 0.125
- upper_transfer: bfloat16 [2, 4, 64, 128], replicated, may hold values from -0.5 to 0.5
- upper_coupling: bfloat16 [2, 5, 64, 256], replicated, may hold values from -0.4375 to 0.4375
- leaf_coupling: bfloat16 [2, 2048, 64, 512], P(None, 'branch'), may hold values from -0.375 to 0.375
- near_blocks: bfloat16 [2, 2048, 4, 256, 256], P(None, 'branch'), may hold values from -0.25 to 0.25
- far_mask: int32 [5, 64, 4], replicated, may hold values 0 or 1
- far_ids: int32 [2048, 8], P('branch'), may hold values from 0 to 2047, as said below
- far_count: int32 [2048], P('branch'), may hold values from 1 to 8
- near_ids: int32 [2048, 4], P('branch'), may hold values from 0 to 2047, as said below
- near_count: int32 [2048], P('branch'), may hold values from 2 to 4, as said below
Outputs:
- sample: bfloat16 [128, 524288], P('col', 'branch')
The draws below stay inside these ranges and needn't reach their ends.
Inputs may be any that keep to these rules, and one draw needn't show every extreme that they name: `near_ids`: entry 0 of leaf i's list is i itself; every entry lies between (i // 32 - 1) * 32 and (i // 32 + 2) * 32 - 1. `far_ids`: every entry of leaf i's list lies between (i // 32 - 1) * 32 and (i // 32 + 2) * 32 - 1. `near_count`: some leaf has 4 live slots.
All inputs are finite; a program needn't handle non-finite values.
Results may differ from the reference program's by a relative error of at most 0.014.
Values may be sent and summed in bfloat16 or wider, within the bound.
A program may use at most 128 MiB of HBM per device.

```python
import jax
import jax.numpy as jnp
from jax import lax

LEAF = 256
RANK = 64
N_VEC = 128
LEAF_DEV = 32
NEAR_MAX = 4
FAR_MAX = 8
LIFTS = 5
LEAVES = 2048
ORDER = 524288
N_BRANCH = 64


def window_ids(key, slots):
    leaf_index = jnp.arange(LEAVES, dtype=jnp.int32)
    first_leaf = leaf_index // LEAF_DEV * LEAF_DEV
    stride = jax.random.randint(key, (LEAVES, slots), -LEAF_DEV, 2 * LEAF_DEV, dtype=jnp.int32)
    return jnp.clip(first_leaf[:, None] + stride, 0, LEAVES - 1).astype(jnp.int32)


def draw_far_ids(key, part):
    return window_ids(jax.random.fold_in(key, 11), FAR_MAX)


def draw_near_ids(key, part):
    listed = window_ids(jax.random.fold_in(key, 13), NEAR_MAX)
    leaf_index = jnp.arange(LEAVES, dtype=jnp.int32)
    first_leaf = leaf_index // LEAF_DEV * LEAF_DEV
    within = jax.random.randint(jax.random.fold_in(key, 19), (LEAVES,), 0, LEAF_DEV, dtype=jnp.int32)
    neighbour_start = jnp.where(leaf_index % 2 == 0, first_leaf - LEAF_DEV, first_leaf + LEAF_DEV)
    neighbour = jnp.clip(neighbour_start + within, 0, LEAVES - 1).astype(jnp.int32)
    listed = listed.at[:, 1].set(neighbour)
    return listed.at[:, 0].set(leaf_index).astype(jnp.int32)


def draw_near_count(key, part):
    subkeys = jax.random.split(jax.random.fold_in(key, 17), 5)
    heaviest = jax.random.randint(subkeys[0], (), 0, N_BRANCH, dtype=jnp.int32)
    lottery = jax.random.randint(subkeys[1], (N_BRANCH,), 0, 4, dtype=jnp.int32)
    lighter = jax.random.randint(subkeys[2], (N_BRANCH,), 2, 3, dtype=jnp.int32)
    deepest = jnp.where(lottery == 0, NEAR_MAX, jnp.minimum(lighter, NEAR_MAX))
    deepest = jnp.where(jnp.arange(N_BRANCH) == heaviest, NEAR_MAX, deepest).astype(jnp.int32)
    counts = jax.random.randint(subkeys[3], (N_BRANCH, LEAF_DEV), 2, NEAR_MAX + 1, dtype=jnp.int32)
    counts = jnp.minimum(counts, deepest[:, None])
    chosen = jax.random.randint(subkeys[4], (N_BRANCH, 1), 0, LEAF_DEV, dtype=jnp.int32)
    counts = jnp.where(jnp.arange(LEAF_DEV)[None, :] == chosen, deepest[:, None], counts)
    return counts.reshape(LEAVES).astype(jnp.int32)


def set_ends(array, stream_key, smallest, largest):
    dims = array.shape
    place = [jax.random.randint(jax.random.fold_in(stream_key, axis), (), 0, dims[axis]) for axis in range(len(dims))]
    array = array.at[tuple(place)].set(smallest)
    longest = dims.index(max(dims))
    place[longest] = (place[longest] + 1) % dims[longest]
    return array.at[tuple(place)].set(largest)


def levels(own_key, dims, cuts, low, largest):
    level = 1.0
    for dim, shards_of in cuts:
        steps = jax.random.uniform(jax.random.fold_in(jax.random.fold_in(own_key, 6), dim), (shards_of,), jnp.float32, low / len(cuts), largest / len(cuts))
        level = level * jnp.repeat(jnp.exp(steps), dims[dim] // shards_of).reshape((-1,) + (1,) * (len(dims) - 1 - dim))
    return level


def scatter_about(key, shape, scale, bound, shards=(), held_as=jnp.bfloat16):
    result = jax.random.normal(key, shape, jnp.float32) * scale
    if len(shards) > 0:
        result = levels(key, shape, shards, -0.22, 0.18) * result
    return jnp.clip(result, min=-bound, max=bound).astype(held_as)


def setup_inputs(seed: int = 0) -> dict:
    keys = jax.random.split(jax.random.key(seed), 13)
    return {
        "vectors": scatter_about(keys[0], (N_VEC, ORDER), 1.0, 6.0, ((0, 4), (1, 64))),
        "basis": scatter_about(keys[1], (2, LEAVES, RANK, LEAF), LEAF ** -0.5, 0.375, ((1, 64),)),
        "leaf_transfer": scatter_about(keys[2], (2, RANK, LEAVES * RANK), (LEAF_DEV * RANK) ** -0.5, 0.125, ((2, 64),)),
        "upper_transfer": scatter_about(keys[3], (2, LIFTS - 1, RANK, 2 * RANK), (2 * RANK) ** -0.5, 0.5),
        "upper_coupling": scatter_about(keys[4], (2, LIFTS, RANK, 4 * RANK), (3 * RANK) ** -0.5, 0.4375),
        "leaf_coupling": scatter_about(keys[5], (2, LEAVES, RANK, FAR_MAX * RANK), (FAR_MAX * RANK // 2) ** -0.5, 0.375, ((1, 64),)),
        "near_blocks": scatter_about(keys[6], (2, LEAVES, NEAR_MAX, LEAF, LEAF), (NEAR_MAX * LEAF // 2) ** -0.5, 0.25, ((1, 64),)),
        "far_mask": set_ends((jax.random.randint(keys[7], (LIFTS, N_BRANCH, 4), 0, 4) < 3).astype(jnp.int32), jax.random.fold_in(keys[7], 1), 0, 1),
        "far_ids": draw_far_ids(jax.random.fold_in(keys[12], 71), 0),
        "far_count": set_ends(jax.random.randint(keys[9], (LEAVES,), 1, FAR_MAX + 1), jax.random.fold_in(keys[9], 1), 1, FAR_MAX).astype(jnp.int32),
        "near_ids": draw_near_ids(jax.random.fold_in(keys[12], 71), 0),
        "near_count": draw_near_count(jax.random.fold_in(keys[12], 71), 0),
    }


OFFSETS = (-3, -2, 2, 3)


def apply_matrix(matrix_index, vectors, basis, leaf_transfer, upper_transfer, upper_coupling, leaf_coupling, near_blocks, far_mask, far_ids, far_count, near_ids, near_count):
    columns = vectors.shape[0]
    leaf_rows = vectors.reshape(columns, LEAVES, LEAF)
    base = basis[matrix_index].astype(jnp.float32)
    leaf_coef = jnp.einsum('ikr,vir->vik', base, leaf_rows.astype(jnp.float32)).astype(jnp.bfloat16)
    spread = leaf_transfer[matrix_index].astype(jnp.float32)
    transfer = spread.reshape(RANK, N_BRANCH, LEAF_DEV * RANK)
    flat_coef = leaf_coef.astype(jnp.float32).reshape(columns, N_BRANCH, LEAF_DEV * RANK)
    lifted = [jnp.einsum('kdj,vdj->vdk', transfer, flat_coef).astype(jnp.bfloat16)]
    for height in range(LIFTS - 1):
        below = lifted[-1].astype(jnp.float32)
        siblings = below.reshape(columns, below.shape[1] // 2, 2 * RANK)
        joined = upper_transfer[matrix_index, height].astype(jnp.float32)
        lifted.append(jnp.einsum('kj,vnj->vnk', joined, siblings).astype(jnp.bfloat16))
    descent = None
    for height in reversed(range(LIFTS)):
        current = lifted[height].astype(jnp.float32)
        nodes = current.shape[1]
        padded = jnp.pad(current, ((0, 0), (3, 3), (0, 0)))
        shifted = jnp.concatenate([padded[:, 3 + offset:3 + offset + nodes] for offset in OFFSETS], axis=2)
        weights = jnp.repeat(far_mask[height, :nodes].astype(jnp.float32), RANK, axis=1)
        coupling = upper_coupling[matrix_index, height].astype(jnp.float32)
        coupled = jnp.einsum('kj,vnj->vnk', coupling, shifted * weights[None])
        if descent is not None:
            parent = lax.optimization_barrier(descent.astype(jnp.bfloat16)).astype(jnp.float32)
            joined = upper_transfer[matrix_index, height].astype(jnp.float32).reshape(RANK, 2, RANK)
            child = jnp.einsum('ksj,vnk->vnsj', joined, parent).reshape(columns, nodes, RANK)
            coupled = coupled + child
        descent = coupled
    parent = lax.optimization_barrier(descent.astype(jnp.bfloat16)).astype(jnp.float32)
    per_leaf = spread.reshape(RANK, N_BRANCH, LEAF_DEV, RANK)
    from_tree = jnp.einsum('kdlj,vdk->vdlj', per_leaf, parent).reshape(columns, LEAVES, RANK)
    far_active = lax.broadcasted_iota(jnp.int32, (LEAVES, FAR_MAX), 1) < far_count[:, None]
    picked = leaf_coef[:, far_ids].astype(jnp.float32) * far_active[None, :, :, None].astype(jnp.float32)
    picked = picked.reshape(columns, LEAVES, FAR_MAX * RANK)
    leaf_field = jnp.einsum('ikj,vij->vik', leaf_coupling[matrix_index].astype(jnp.float32), picked) + from_tree
    leaf_round = lax.optimization_barrier(leaf_field.astype(jnp.bfloat16)).astype(jnp.float32)
    far_terms = jnp.einsum('ikr,vik->vir', base, leaf_round)
    near_active = lax.broadcasted_iota(jnp.int32, (LEAVES, NEAR_MAX), 1) < near_count[:, None]
    sources = leaf_rows[:, near_ids] * near_active[None, :, :, None].astype(jnp.bfloat16)

    def one_leaf(pieces):
        dense, inputs = pieces
        return jnp.einsum('jrc,vjc->vr', dense.astype(jnp.float32), inputs.astype(jnp.float32))

    near_terms = lax.map(one_leaf, (near_blocks[matrix_index], jnp.moveaxis(sources, 1, 0)))
    near_terms = jnp.moveaxis(near_terms, 0, 1)
    return (near_terms + far_terms).astype(jnp.bfloat16).reshape(columns, LEAVES * LEAF)


def reference(vectors, basis, leaf_transfer, upper_transfer, upper_coupling, leaf_coupling, near_blocks, far_mask, far_ids, far_count, near_ids, near_count):
    first = apply_matrix(0, vectors, basis, leaf_transfer, upper_transfer, upper_coupling, leaf_coupling, near_blocks, far_mask, far_ids, far_count, near_ids, near_count)
    return apply_matrix(1, first, basis, leaf_transfer, upper_transfer, upper_coupling, leaf_coupling, near_blocks, far_mask, far_ids, far_count, near_ids, near_count)
```

```python
import jax
import jax.numpy as jnp
from jax import lax
from jax.experimental import pallas as pl
from jax.experimental.pallas import tpu as pltpu
from jax.sharding import PartitionSpec as P

OFFSETS = (-3, -2, 2, 3)
PLANE = 8
PLANES = 8
LEAF_DEV = 32
LEAF = 256
RANK = 64
COLS = 32
CHUNKS = 8
NT = (((1,), (1,)), ((), ()))
NN = (((1,), (0,)), ((), ()))


def dot_nt(a, b):
    return lax.dot_general(a, b, NT, preferred_element_type=jnp.float32)


def dot_nn(a, b):
    return lax.dot_general(a, b, NN, preferred_element_type=jnp.float32)


def kernel(
    far_mask, far_ids, far_count, near_ids, near_count,
    vectors, basis, leaf_transfer, upper_transfer, upper_coupling, leaf_coupling, near_blocks,
    out,
    near_w, coup_w, basis_w, trans_w, up_t, up_c,
    va, vb, cpa, cpb, dl, dr, near_acc, field,
    l0, l1, l2, l3, l4, cc,
    sem_near, sem_in,
    v_send, v_recv, c_send, c_recv, p_send, p_recv, z_send, z_recv, e_send, e_recv,
):
    b = lax.axis_index("branch")
    col = lax.axis_index("col")
    z = b // PLANE
    j = lax.rem(b, PLANE)
    core = lax.rem(b, 2)
    x = j // 2
    first_leaf = (b - 1) * LEAF_DEV
    lane = lax.broadcasted_iota(jnp.int32, (COLS, 128), 1)
    left = lane < 64

    def local(src, dst, sem):
        copy = pltpu.make_async_copy(src, dst, sem)
        copy.start()
        return copy

    def load_leaf(i, carry):
        local(vectors.at[:, pl.ds(pl.multiple_of(i * LEAF, LEAF), LEAF)], va.at[LEAF_DEV + i], sem_in.at[0])
        return carry

    lax.fori_loop(0, LEAF_DEV, load_leaf, 0, unroll=4)
    own = pl.ds(LEAF_DEV, LEAF_DEV)
    load_v = pltpu.make_async_copy(va.at[own], va.at[own], sem_in.at[0])
    load_basis = [None, None]
    load_trans = [None, None]
    load_coup = [None, None]
    load_near = [[], []]
    load_basis[0] = local(basis.at[0], basis_w.at[0], sem_in.at[1])
    load_trans[0] = local(leaf_transfer.at[0], trans_w.at[0], sem_in.at[2])
    load_ut = local(upper_transfer, up_t, sem_in.at[3])
    load_uc = local(upper_coupling, up_c, sem_in.at[4])
    step = LEAF_DEV // CHUNKS
    for m in range(2):
        if m == 1:
            load_basis[1] = local(basis.at[1], basis_w.at[1], sem_in.at[5])
            load_trans[1] = local(leaf_transfer.at[1], trans_w.at[1], sem_in.at[6])
        for g in range(CHUNKS):
            part = pl.ds(g * step, step)
            load_near[m].append(local(near_blocks.at[m, part], near_w.at[m, part], sem_near.at[m, g]))
            if g == 1:
                load_coup[m] = local(leaf_coupling.at[m], coup_w.at[m], sem_in.at[7 + m])

    barrier = pltpu.get_barrier_semaphore()

    def greet(target):
        pl.semaphore_signal(barrier, inc=1, device_id=(target, col), device_id_type=pl.DeviceIdType.MESH)

    plane_peer = [z * PLANE + lax.rem(j + d, PLANE) for d in range(PLANE)]
    z_peer = [lax.rem(z + d, PLANES) * PLANE + j for d in range(PLANES)]

    @pl.when(b > 0)
    def _():
        greet(b - 1)

    @pl.when(b < PLANE * PLANES - 1)
    def _():
        greet(b + 1)

    for d in range(1, PLANE):
        greet(plane_peer[d])
    for d in range(1, PLANES):
        greet(z_peer[d])

    va[96] = jnp.zeros((COLS, LEAF), jnp.bfloat16)
    vb[96] = jnp.zeros((COLS, LEAF), jnp.bfloat16)
    dl[96] = jnp.zeros((COLS, 128), jnp.bfloat16)
    dr[96] = jnp.zeros((COLS, 128), jnp.bfloat16)

    def remote(src, dst, send, recv, target):
        return pltpu.make_async_remote_copy(
            src_ref=src, dst_ref=dst, send_sem=send, recv_sem=recv,
            device_id=(target, col), device_id_type=pl.DeviceIdType.MESH,
        )

    def halo_sends(m, mine, to_right, to_left, send, recv):
        return (
            remote(mine, to_right, send.at[m, 0], recv.at[m, 0], b + 1),
            remote(mine, to_left, send.at[m, 1], recv.at[m, 1], b - 1),
        )

    has_right = b < PLANE * PLANES - 1
    has_left = b > 0

    def halo_start(copies):
        @pl.when(has_right)
        def _():
            copies[0].start()

        @pl.when(has_left)
        def _():
            copies[1].start()

    def halo_recv(copies):
        @pl.when(has_left)
        def _():
            copies[0].wait_recv()

        @pl.when(has_right)
        def _():
            copies[1].wait_recv()

    def halo_sent(copies):
        @pl.when(has_right)
        def _():
            copies[0].wait_send()

        @pl.when(has_left)
        def _():
            copies[1].wait_send()

    def halves(pair):
        turned = pltpu.roll(pair, 64, 1)
        none = jnp.zeros_like(pair)
        return (
            jnp.where(left, pair, none).astype(jnp.bfloat16),
            jnp.where(left, none, turned).astype(jnp.bfloat16),
            jnp.where(left, turned, none).astype(jnp.bfloat16),
            jnp.where(left, none, pair).astype(jnp.bfloat16),
        )

    def put_halves(leaf, pair):
        al, ar, bl, br = halves(pair)
        dl[leaf] = al
        dr[leaf] = ar
        dl[leaf + 1] = bl
        dr[leaf + 1] = br

    def coef_pair(m, source, cp, p):
        lhs = source[pl.ds(LEAF_DEV + 2 * p, 2)].reshape(2 * COLS, LEAF)
        rhs = basis_w[m, pl.ds(2 * p, 2)].reshape(128, LEAF)
        both = dot_nt(lhs, rhs)
        got = jnp.where(left, both[:COLS], both[COLS:])
        cp[:, pl.ds(pl.multiple_of(LEAF_DEV * RANK + p * 128, 128), 128)] = got.astype(jnp.bfloat16)
        put_halves(LEAF_DEV + 2 * p, got)

    def masked_half(both, parity):
        keep = jnp.logical_xor(left, parity == 1)
        return jnp.where(keep, both, jnp.zeros_like(both)).astype(jnp.bfloat16)

    def live_or_zero(q, count, leaf):
        dead = lax.shift_right_arithmetic(q - count, 31) + 1
        return (leaf - first_leaf) + dead * (96 - (leaf - first_leaf))

    for m in range(2):
        source = va if m == 0 else vb
        cp = cpa if m == 0 else cpb
        if m == 0:
            load_v.wait()
            load_basis[0].wait()

            def coef_body(p, carry):
                coef_pair(0, va, cpa, p)
                return carry

            lax.fori_loop(0, LEAF_DEV // 2, coef_body, 0, unroll=2)
        load_trans[m].wait()
        box = dot_nt(cp[:, pl.ds(LEAF_DEV * RANK, LEAF_DEV * RANK)], trans_w[m])
        l0[m, 3 + j] = masked_half(jnp.concatenate([box, box], axis=1), core)
        if m == 0:
            last = PLANE * PLANES - 1
            pl.semaphore_wait(barrier, 14 + (b + last) // (last + 1) + (2 * last - b) // (last + 1))
        plane = []
        for d in range(1, PLANE):
            copy = remote(l0.at[m, 3 + j], l0.at[m, 3 + j], p_send.at[m, d], p_recv.at[m, d], plane_peer[d])
            copy.start()
            plane.append(copy)
        flat = LEAF_DEV * RANK
        coef_halo = halo_sends(
            m, cp.at[:, pl.ds(flat, flat)], cp.at[:, pl.ds(0, flat)], cp.at[:, pl.ds(2 * flat, flat)], c_send, c_recv
        )
        halo_start(coef_halo)
        vec_halo = halo_sends(
            m, source.at[own], source.at[pl.ds(0, LEAF_DEV)], source.at[pl.ds(2 * LEAF_DEV, LEAF_DEV)], v_send, v_recv
        )
        halo_start(vec_halo)

        if m == 0:
            load_ut.wait()
            load_uc.wait()
            for mm in range(2):
                for h in range(5):
                    blocks = []
                    for q in range(4):
                        one = up_c[mm, h, :, q * RANK:(q + 1) * RANK]
                        blocks += [one, one]
                    cc[mm, h] = jnp.concatenate(blocks, axis=1)

        for g in range(CHUNKS):
            load_near[m][g].wait()

        def own_body(i, carry):
            piece = source[LEAF_DEV + i]
            near_acc[:, pl.ds(pl.multiple_of(i * LEAF, LEAF), LEAF)] = dot_nt(piece, near_w[m, i, 0])
            return carry

        lax.fori_loop(0, LEAF_DEV, own_body, 0, unroll=2)

        for copy in plane:
            copy.wait_recv()

        def lift(pairs, h):
            weight = up_t[m, h]
            return dot_nt(pairs, jnp.concatenate([weight, weight], axis=0))

        pairs = jnp.concatenate([l0[m, 3 + 2 * i] + l0[m, 4 + 2 * i] for i in range(4)], axis=0)
        lifted = lift(pairs, 0)
        n1 = [masked_half(lifted[i * COLS:(i + 1) * COLS], i % 2) for i in range(4)]
        for i in range(4):
            l1[m, 3 + i] = n1[i]
        lifted = lift(jnp.concatenate([n1[0] + n1[1], n1[2] + n1[3]], axis=0), 1)
        n2 = [masked_half(lifted[i * COLS:(i + 1) * COLS], i % 2) for i in range(2)]
        for i in range(2):
            l2[m, 4 + i] = n2[i]
        l3[m, z] = masked_half(lift(n2[0] + n2[1], 2), lax.rem(z, 2))

        across = []
        for d in range(1, PLANES):
            copy = remote(l3.at[m, z], l3.at[m, z], z_send.at[m, d], z_recv.at[m, d], z_peer[d])
            copy.start()
            across.append(copy)
        up_one = b + PLANE
        down_one = b - PLANE
        up_two = b + 2 * PLANE
        down_two = b - 2 * PLANE

        def edge(k, src, dst, target):
            return remote(src, dst, e_send.at[m, k], e_recv.at[m, k], target)

        ups = [
            edge(0, l2.at[m, pl.ds(4, 2)], l2.at[m, pl.ds(2, 2)], up_one),
            edge(1, l1.at[m, pl.ds(4, 3)], l1.at[m, pl.ds(0, 3)], up_one),
            edge(2, l0.at[m, pl.ds(8, 3)], l0.at[m, pl.ds(0, 3)], up_one),
        ]
        downs = [
            edge(3, l2.at[m, pl.ds(4, 2)], l2.at[m, pl.ds(6, 2)], down_one),
            edge(4, l1.at[m, pl.ds(3, 3)], l1.at[m, pl.ds(7, 3)], down_one),
            edge(5, l0.at[m, pl.ds(3, 3)], l0.at[m, pl.ds(11, 3)], down_one),
        ]
        up2 = edge(6, l2.at[m, pl.ds(4, 2)], l2.at[m, pl.ds(0, 2)], up_two)
        down2 = edge(7, l2.at[m, pl.ds(4, 2)], l2.at[m, pl.ds(8, 2)], down_two)

        @pl.when(z + 1 < PLANES)
        def _():
            for copy in ups:
                copy.start()

        @pl.when(z > 0)
        def _():
            for copy in downs:
                copy.start()

        @pl.when(z + 2 < PLANES)
        def _():
            up2.start()

        @pl.when(z > 1)
        def _():
            down2.start()

        halo_recv(coef_halo)

        def dup_body(p, carry):
            for spot in (p, p + LEAF_DEV):
                pair = cp[:, pl.ds(pl.multiple_of(spot * 128, 128), 128)].astype(jnp.float32)
                put_halves(2 * spot, pair)
            return carry

        lax.fori_loop(0, LEAF_DEV // 2, dup_body, 0)
        load_coup[m].wait()

        def far_rows(i):
            count = far_count[i]

            def spot(q):
                return live_or_zero(q, count, far_ids[q, i])

            return jnp.concatenate([dl[spot(2 * t)] + dr[spot(2 * t + 1)] for t in range(4)], axis=1)

        def coup_body(p, carry):
            lhs = jnp.concatenate([far_rows(2 * p), far_rows(2 * p + 1)], axis=0)
            rhs = coup_w[m, pl.ds(2 * p, 2)].reshape(128, 512)
            both = dot_nt(lhs, rhs)
            field[:, pl.ds(pl.multiple_of(p * 128, 128), 128)] = jnp.where(left, both[:COLS], both[COLS:])
            return carry

        lax.fori_loop(0, LEAF_DEV // 2, coup_body, 0, unroll=1)

        halo_recv(vec_halo)

        def near_body(i, carry):
            where_to = pl.ds(pl.multiple_of(i * LEAF, LEAF), LEAF)
            total = near_acc[:, where_to]
            count = near_count[i]
            for q in range(1, 4):
                spot = live_or_zero(q, count, near_ids[q, i])
                piece = source[spot]
                total = total + dot_nt(piece, near_w[m, i, q])
            near_acc[:, where_to] = total
            return carry

        lax.fori_loop(0, LEAF_DEV, near_body, 0, unroll=2)

        for copy in across:
            copy.wait_recv()

        @pl.when(z + 1 < PLANES)
        def _():
            for copy in downs:
                copy.wait_recv()

        @pl.when(z > 0)
        def _():
            for copy in ups:
                copy.wait_recv()

        @pl.when(z + 2 < PLANES)
        def _():
            down2.wait_recv()

        @pl.when(z > 1)
        def _():
            up2.wait_recv()

        pairs = jnp.concatenate([l3[m, 2 * i] + l3[m, 2 * i + 1] for i in range(4)], axis=0)
        lifted = lift(pairs, 3)
        for i in range(4):
            l4[i] = masked_half(lifted[i * COLS:(i + 1) * COLS], 0)

        def node(h, o):
            if h == 0:
                return l0[m, 3 + j + o]
            if h == 1:
                return l1[m, 3 + x + o]
            if h == 2:
                return l2[m, 4 + x // 2 + o]
            if h == 3:
                return l3[m, lax.rem(z + o + PLANES, PLANES)]
            return l4[lax.rem(z // 2 + o + 4, 4)]

        def coupled(h):
            n = b // (1 << h)
            blocks = []
            for q, o in enumerate(OFFSETS):
                there = jnp.logical_and(n + o >= 0, n + o < (64 >> h))
                live = jnp.full((COLS, 128), far_mask[h, q, n].astype(jnp.float32)).astype(jnp.bfloat16)
                blocks.append(jnp.where(there, node(h, o), jnp.zeros((COLS, 128), jnp.bfloat16)) * live)
            return dot_nt(jnp.concatenate(blocks, axis=1), cc[m, h])

        descent = coupled(4)
        for h in (3, 2, 1, 0):
            both = dot_nn(descent.astype(jnp.bfloat16), up_t[m, h])
            side = lax.rem(b // (1 << h), 2)
            descent = coupled(h) + jnp.where(side == 0, both[:, :RANK], both[:, RANK:])
        parent = descent.astype(jnp.bfloat16)
        field[...] += dot_nn(parent, trans_w[m])

        def final_body(p, carry):
            pair = field[:, pl.ds(pl.multiple_of(p * 128, 128), 128)]
            none = jnp.zeros_like(pair)
            lhs = jnp.concatenate([jnp.where(left, pair, none), jnp.where(left, none, pair)], axis=0).astype(jnp.bfloat16)
            rhs = basis_w[m, pl.ds(2 * p, 2)].reshape(128, LEAF)
            both = dot_nn(lhs, rhs)
            total = near_acc[:, pl.ds(pl.multiple_of(p * 512, 512), 512)]
            first = (total[:, :LEAF] + both[:COLS]).astype(jnp.bfloat16)
            second = (total[:, LEAF:] + both[COLS:]).astype(jnp.bfloat16)
            if m == 0:
                vb[LEAF_DEV + 2 * p] = first
                vb[LEAF_DEV + 2 * p + 1] = second
                coef_pair(1, vb, cpb, p)
            else:
                out[:, pl.ds(pl.multiple_of(p * 512, 512), LEAF)] = first
                out[:, pl.ds(pl.multiple_of(p * 512 + LEAF, LEAF), LEAF)] = second
            return carry

        if m == 0:
            load_basis[1].wait()
        lax.fori_loop(0, LEAF_DEV // 2, final_body, 0, unroll=2)

        for copy in plane + across:
            copy.wait_send()
        halo_sent(coef_halo)
        halo_sent(vec_halo)

        @pl.when(z + 1 < PLANES)
        def _():
            for copy in ups:
                copy.wait_send()

        @pl.when(z > 0)
        def _():
            for copy in downs:
                copy.wait_send()

        @pl.when(z + 2 < PLANES)
        def _():
            up2.wait_send()

        @pl.when(z > 1)
        def _():
            down2.wait_send()


def shards(
    vectors, basis, leaf_transfer, upper_transfer, upper_coupling, leaf_coupling, near_blocks,
    far_mask, far_ids, far_count, near_ids, near_count,
):
    smem = pl.BlockSpec(memory_space=pltpu.SMEM)
    hbm = pl.BlockSpec(memory_space=pl.ANY)
    bf = jnp.bfloat16
    f32 = jnp.float32
    dma = pltpu.SemaphoreType.DMA
    return pl.pallas_call(
        kernel,
        out_shape=jax.ShapeDtypeStruct((COLS, LEAF_DEV * LEAF), bf),
        in_specs=[smem] * 5 + [hbm] * 7,
        out_specs=pl.BlockSpec(memory_space=pltpu.VMEM),
        scratch_shapes=[
            pltpu.VMEM((2, LEAF_DEV, 4, LEAF, LEAF), bf),
            pltpu.VMEM((2, LEAF_DEV, RANK, 512), bf),
            pltpu.VMEM((2, LEAF_DEV, RANK, LEAF), bf),
            pltpu.VMEM((2, RANK, LEAF_DEV * RANK), bf),
            pltpu.VMEM((2, 4, RANK, 128), bf),
            pltpu.VMEM((2, 5, RANK, 256), bf),
            pltpu.VMEM((97, COLS, LEAF), bf),
            pltpu.VMEM((97, COLS, LEAF), bf),
            pltpu.VMEM((COLS, 96 * RANK), bf),
            pltpu.VMEM((COLS, 96 * RANK), bf),
            pltpu.VMEM((97, COLS, 128), bf),
            pltpu.VMEM((97, COLS, 128), bf),
            pltpu.VMEM((COLS, LEAF_DEV * LEAF), f32),
            pltpu.VMEM((COLS, LEAF_DEV * RANK), f32),
            pltpu.VMEM((2, 14, COLS, 128), bf),
            pltpu.VMEM((2, 10, COLS, 128), bf),
            pltpu.VMEM((2, 10, COLS, 128), bf),
            pltpu.VMEM((2, 8, COLS, 128), bf),
            pltpu.VMEM((4, COLS, 128), bf),
            pltpu.VMEM((2, 5, RANK, 512), bf),
            dma((2, CHUNKS)), dma((9,)),
            dma((2, 2)), dma((2, 2)), dma((2, 2)), dma((2, 2)),
            dma((2, 8)), dma((2, 8)), dma((2, 8)), dma((2, 8)), dma((2, 8)), dma((2, 8)),
        ],
        compiler_params=pltpu.CompilerParams(
            collective_id=0, has_side_effects=True, vmem_limit_bytes=60 << 20
        ),
        name="product",
    )(
        jnp.transpose(far_mask, (0, 2, 1)), far_ids.T, far_count, near_ids.T, near_count,
        vectors, basis, leaf_transfer, upper_transfer, upper_coupling, leaf_coupling, near_blocks,
    )


def solution(mesh):
    return jax.shard_map(
        shards,
        mesh=mesh,
        in_specs=(
            P("col", "branch"),
            P(None, "branch", None, None),
            P(None, None, "branch"),
            P(),
            P(),
            P(None, "branch", None, None),
            P(None, "branch", None, None, None),
            P(),
            P("branch", None),
            P("branch"),
            P("branch", None),
            P("branch"),
        ),
        out_specs=P("col", "branch"),
        check_vma=False,
    )
```

```python
import jax
import jax.numpy as jnp
from jax import lax
from jax.experimental import pallas as pl
from jax.experimental.pallas import tpu as pltpu
from jax.sharding import PartitionSpec as P

OFFSETS = (-3, -2, 2, 3)
PLANE = 8
PLANES = 8
LEAF_DEV = 32
LEAF = 256
RANK = 64
COLS = 32
CHUNKS = 8
STEP = LEAF_DEV // CHUNKS
HELD = 2
NT = (((1,), (1,)), ((), ()))
NN = (((1,), (0,)), ((), ()))


def dot_nt(a, b):
    return lax.dot_general(a, b, NT, preferred_element_type=jnp.float32)


def dot_nn(a, b):
    return lax.dot_general(a, b, NN, preferred_element_type=jnp.float32)


def kernel(
    far_mask_in, far_ids_in, far_count_in, near_ids_in, near_count_in,
    vectors, basis, leaf_transfer, upper_transfer, upper_coupling, leaf_coupling, near_blocks,
    out,
    far_mask, far_ids, far_count, near_ids, near_count,
    near_w, coup_w, basis_w, trans_w, up_t, up_c,
    va, vb, cpa, cpb, dl, dr, near_acc, field,
    l0, l1, l2, l3, l4, cc,
    sem_near, sem_in, sem_small,
    v_send, v_recv, c_send, c_recv, p_send, p_recv, z_send, z_recv, e_send, e_recv,
):
    b = lax.axis_index("branch")
    col = lax.axis_index("col")
    z = b // PLANE
    j = lax.rem(b, PLANE)
    core = lax.rem(b, 2)
    x = j // 2
    first_leaf = (b - 1) * LEAF_DEV
    lane = lax.broadcasted_iota(jnp.int32, (COLS, 128), 1)
    left = lane < 64

    def local(src, dst, sem):
        copy = pltpu.make_async_copy(src, dst, sem)
        copy.start()
        return copy

    def load_leaf(i, carry):
        local(vectors.at[:, pl.ds(pl.multiple_of(i * LEAF, LEAF), LEAF)], va.at[LEAF_DEV + i], sem_in.at[0])
        return carry

    lax.fori_loop(0, LEAF_DEV, load_leaf, 0, unroll=4)
    own = pl.ds(LEAF_DEV, LEAF_DEV)
    load_v = pltpu.make_async_copy(va.at[own], va.at[own], sem_in.at[0])
    load_basis = [None, None]
    load_trans = [None, None]
    load_coup = [None, None]
    load_near = [[], []]
    load_basis[0] = local(basis.at[0], basis_w.at[0], sem_in.at[1])
    load_trans[0] = local(leaf_transfer.at[0], trans_w.at[0], sem_in.at[2])
    load_ut = local(upper_transfer, up_t, sem_in.at[3])
    load_uc = local(upper_coupling, up_c, sem_in.at[4])
    load_small = [
        local(far_mask_in, far_mask, sem_small.at[0]),
        local(far_ids_in, far_ids, sem_small.at[1]),
        local(far_count_in, far_count, sem_small.at[2]),
        local(near_ids_in, near_ids, sem_small.at[3]),
        local(near_count_in, near_count, sem_small.at[4]),
    ]
    for m in range(2):
        if m == 1:
            load_basis[1] = local(basis.at[1], basis_w.at[1], sem_in.at[5])
            load_trans[1] = local(leaf_transfer.at[1], trans_w.at[1], sem_in.at[6])
        for g in range(2):
            part = pl.ds(g * 16, 16)
            load_near[m].append(local(near_blocks.at[m, part, 0], near_w.at[m, part, 0], sem_near.at[m, g]))
        load_coup[m] = local(leaf_coupling.at[m], coup_w.at[m], sem_in.at[7 + m])
        for g in range(6):
            part = pl.ds((g % 2) * 16, 16)
            slot = 1 + g // 2
            load_near[m].append(local(near_blocks.at[m, part, slot], near_w.at[m, part, slot], sem_near.at[m, 2 + g]))

    barrier = pltpu.get_barrier_semaphore()

    def greet(target):
        pl.semaphore_signal(barrier, inc=1, device_id=(target, col), device_id_type=pl.DeviceIdType.MESH)

    plane_peer = [z * PLANE + lax.rem(j + d, PLANE) for d in range(PLANE)]
    z_peer = [lax.rem(z + d, PLANES) * PLANE + j for d in range(PLANES)]

    @pl.when(b > 0)
    def _():
        greet(b - 1)

    @pl.when(b < PLANE * PLANES - 1)
    def _():
        greet(b + 1)

    for d in range(1, PLANE):
        greet(plane_peer[d])
    for d in range(1, PLANES):
        greet(z_peer[d])

    va[96] = jnp.zeros((COLS, LEAF), jnp.bfloat16)
    vb[96] = jnp.zeros((COLS, LEAF), jnp.bfloat16)
    dl[96] = jnp.zeros((COLS, 128), jnp.bfloat16)
    dr[96] = jnp.zeros((COLS, 128), jnp.bfloat16)

    def remote(src, dst, send, recv, target):
        return pltpu.make_async_remote_copy(
            src_ref=src, dst_ref=dst, send_sem=send, recv_sem=recv,
            device_id=(target, col), device_id_type=pl.DeviceIdType.MESH,
        )

    def halo_sends(m, mine, to_right, to_left, send, recv):
        return (
            remote(mine, to_right, send.at[m, 0], recv.at[m, 0], b + 1),
            remote(mine, to_left, send.at[m, 1], recv.at[m, 1], b - 1),
        )

    has_right = b < PLANE * PLANES - 1
    has_left = b > 0

    def halo_start(copies):
        @pl.when(has_right)
        def _():
            copies[0].start()

        @pl.when(has_left)
        def _():
            copies[1].start()

    def halo_recv(copies):
        @pl.when(has_left)
        def _():
            copies[0].wait_recv()

        @pl.when(has_right)
        def _():
            copies[1].wait_recv()

    def halo_sent(copies):
        @pl.when(has_right)
        def _():
            copies[0].wait_send()

        @pl.when(has_left)
        def _():
            copies[1].wait_send()

    def halves(pair):
        turned = pltpu.roll(pair, 64, 1)
        none = jnp.zeros_like(pair)
        return (
            jnp.where(left, pair, none).astype(jnp.bfloat16),
            jnp.where(left, none, turned).astype(jnp.bfloat16),
            jnp.where(left, turned, none).astype(jnp.bfloat16),
            jnp.where(left, none, pair).astype(jnp.bfloat16),
        )

    def put_halves(leaf, pair):
        al, ar, bl, br = halves(pair)
        dl[leaf] = al
        dr[leaf] = ar
        dl[leaf + 1] = bl
        dr[leaf + 1] = br

    def coef_pair(m, source, cp, p):
        lhs = source[pl.ds(LEAF_DEV + 2 * p, 2)].reshape(2 * COLS, LEAF)
        rhs = basis_w[m, pl.ds(2 * p, 2)].reshape(128, LEAF)
        both = dot_nt(lhs, rhs)
        got = jnp.where(left, both[:COLS], both[COLS:])
        cp[:, pl.ds(pl.multiple_of(LEAF_DEV * RANK + p * 128, 128), 128)] = got.astype(jnp.bfloat16)
        put_halves(LEAF_DEV + 2 * p, got)

    def masked_half(both, parity):
        keep = jnp.logical_xor(left, parity == 1)
        return jnp.where(keep, both, jnp.zeros_like(both)).astype(jnp.bfloat16)

    def live_or_zero(q, count, leaf):
        dead = lax.shift_right_arithmetic(q - count, 31) + 1
        return (leaf - first_leaf) + dead * (96 - (leaf - first_leaf))

    def far_rows(i):
        count = far_count[i]

        def spot(q):
            return live_or_zero(q, count, far_ids[q, i])

        return jnp.concatenate([dl[spot(2 * t)] + dr[spot(2 * t + 1)] for t in range(4)], axis=1)

    def near_rest(m, source, i):
        total = near_acc[:, pl.ds(pl.multiple_of(i * LEAF, LEAF), LEAF)]
        count = near_count[i]
        for q in range(1, 4):
            piece = source[live_or_zero(q, count, near_ids[q, i])]
            total = total + dot_nt(piece, near_w[m, i, q])
        return total

    def far_terms(m, p):
        pair = field[:, pl.ds(pl.multiple_of(p * 128, 128), 128)]
        none = jnp.zeros_like(pair)
        lhs = jnp.concatenate([jnp.where(left, pair, none), jnp.where(left, none, pair)], axis=0).astype(jnp.bfloat16)
        rhs = basis_w[m, pl.ds(2 * p, 2)].reshape(128, LEAF)
        both = dot_nn(lhs, rhs)
        return both[:COLS], both[COLS:]

    def start_chunk(g):
        copies = halo_sends(
            1,
            vb.at[pl.ds(LEAF_DEV + g * STEP, STEP)],
            vb.at[pl.ds(g * STEP, STEP)],
            vb.at[pl.ds(2 * LEAF_DEV + g * STEP, STEP)],
            v_send, v_recv,
        )
        halo_start(copies)

    for m in range(2):
        source = va if m == 0 else vb
        cp = cpa if m == 0 else cpb
        if m == 0:
            load_v.wait()
            load_basis[0].wait()

            def coef_body(p, carry):
                coef_pair(0, va, cpa, p)
                return carry

            lax.fori_loop(0, LEAF_DEV // 2, coef_body, 0, unroll=4)
        load_trans[m].wait()
        box = dot_nt(cp[:, pl.ds(LEAF_DEV * RANK, LEAF_DEV * RANK)], trans_w[m])
        l0[m, 3 + j] = masked_half(jnp.concatenate([box, box], axis=1), core)
        if m == 0:
            last = PLANE * PLANES - 1
            pl.semaphore_wait(barrier, 14 + (b + last) // (last + 1) + (2 * last - b) // (last + 1))
        plane = []
        for d in range(1, PLANE):
            copy = remote(l0.at[m, 3 + j], l0.at[m, 3 + j], p_send.at[m, d], p_recv.at[m, d], plane_peer[d])
            copy.start()
            plane.append(copy)
        flat = LEAF_DEV * RANK
        coef_halo = halo_sends(
            m, cp.at[:, pl.ds(flat, flat)], cp.at[:, pl.ds(0, flat)], cp.at[:, pl.ds(2 * flat, flat)], c_send, c_recv
        )
        halo_start(coef_halo)
        vec_halo = halo_sends(
            m, source.at[own], source.at[pl.ds(0, LEAF_DEV)], source.at[pl.ds(2 * LEAF_DEV, LEAF_DEV)], v_send, v_recv
        )
        if m == 0:
            halo_start(vec_halo)
        else:
            for g in range(CHUNKS - HELD, CHUNKS):
                start_chunk(g)

        if m == 0:
            for copy in load_small:
                copy.wait()
            load_ut.wait()
            load_uc.wait()
            for mm in range(2):
                for h in range(5):
                    blocks = []
                    for q in range(4):
                        one = up_c[mm, h, :, q * RANK:(q + 1) * RANK]
                        blocks += [one, one]
                    cc[mm, h] = jnp.concatenate(blocks, axis=1)

        for copy in load_near[m][:2]:
            copy.wait()

        def own_body(i, carry):
            near_acc[:, pl.ds(pl.multiple_of(i * LEAF, LEAF), LEAF)] = dot_nt(source[LEAF_DEV + i], near_w[m, i, 0])
            return carry

        lax.fori_loop(0, LEAF_DEV, own_body, 0, unroll=8)

        for copy in plane:
            copy.wait_recv()

        def lift(pairs, h):
            weight = up_t[m, h]
            return dot_nt(pairs, jnp.concatenate([weight, weight], axis=0))

        pairs = jnp.concatenate([l0[m, 3 + 2 * i] + l0[m, 4 + 2 * i] for i in range(4)], axis=0)
        lifted = lift(pairs, 0)
        n1 = [masked_half(lifted[i * COLS:(i + 1) * COLS], i % 2) for i in range(4)]
        for i in range(4):
            l1[m, 3 + i] = n1[i]
        lifted = lift(jnp.concatenate([n1[0] + n1[1], n1[2] + n1[3]], axis=0), 1)
        n2 = [masked_half(lifted[i * COLS:(i + 1) * COLS], i % 2) for i in range(2)]
        for i in range(2):
            l2[m, 4 + i] = n2[i]
        l3[m, z] = masked_half(lift(n2[0] + n2[1], 2), lax.rem(z, 2))

        across = [None]
        for d in range(1, PLANES):
            across.append(remote(l3.at[m, z], l3.at[m, z], z_send.at[m, d], z_recv.at[m, d], z_peer[d]))
        for d in (4, 3, 5, 2, 6, 1, 7):
            across[d].start()
        across = across[1:]
        up_one = b + PLANE
        down_one = b - PLANE
        up_two = b + 2 * PLANE
        down_two = b - 2 * PLANE

        def edge(k, src, dst, target):
            return remote(src, dst, e_send.at[m, k], e_recv.at[m, k], target)

        ups = [
            edge(0, l2.at[m, pl.ds(4, 2)], l2.at[m, pl.ds(2, 2)], up_one),
            edge(1, l1.at[m, pl.ds(4, 3)], l1.at[m, pl.ds(0, 3)], up_one),
            edge(2, l0.at[m, pl.ds(8, 3)], l0.at[m, pl.ds(0, 3)], up_one),
        ]
        downs = [
            edge(3, l2.at[m, pl.ds(4, 2)], l2.at[m, pl.ds(6, 2)], down_one),
            edge(4, l1.at[m, pl.ds(3, 3)], l1.at[m, pl.ds(7, 3)], down_one),
            edge(5, l0.at[m, pl.ds(3, 3)], l0.at[m, pl.ds(11, 3)], down_one),
        ]
        up2 = edge(6, l2.at[m, pl.ds(4, 2)], l2.at[m, pl.ds(0, 2)], up_two)
        down2 = edge(7, l2.at[m, pl.ds(4, 2)], l2.at[m, pl.ds(8, 2)], down_two)

        @pl.when(z + 1 < PLANES)
        def _():
            for copy in ups:
                copy.start()

        @pl.when(z > 0)
        def _():
            for copy in downs:
                copy.start()

        @pl.when(z + 2 < PLANES)
        def _():
            up2.start()

        @pl.when(z > 1)
        def _():
            down2.start()

        halo_recv(coef_halo)

        def dup_body(p, carry):
            for spot in (p, p + LEAF_DEV):
                pair = cp[:, pl.ds(pl.multiple_of(spot * 128, 128), 128)].astype(jnp.float32)
                put_halves(2 * spot, pair)
            return carry

        lax.fori_loop(0, LEAF_DEV // 2, dup_body, 0, unroll=4)
        load_coup[m].wait()

        def coup_body(p, carry):
            lhs = jnp.concatenate([far_rows(2 * p), far_rows(2 * p + 1)], axis=0)
            rhs = coup_w[m, pl.ds(2 * p, 2)].reshape(128, 512)
            both = dot_nt(lhs, rhs)
            field[:, pl.ds(pl.multiple_of(p * 128, 128), 128)] = jnp.where(left, both[:COLS], both[COLS:])
            return carry

        lax.fori_loop(0, LEAF_DEV // 2, coup_body, 0, unroll=4)

        for copy in load_near[m][2:]:
            copy.wait()
        if m == 1:
            halo_recv(vec_halo)

            def near_body(i, carry):
                near_acc[:, pl.ds(pl.multiple_of(i * LEAF, LEAF), LEAF)] = near_rest(m, source, i)
                return carry

            lax.fori_loop(0, LEAF_DEV, near_body, 0, unroll=4)

        @pl.when(z + 1 < PLANES)
        def _():
            for copy in downs:
                copy.wait_recv()

        @pl.when(z > 0)
        def _():
            for copy in ups:
                copy.wait_recv()

        @pl.when(z + 2 < PLANES)
        def _():
            down2.wait_recv()

        @pl.when(z > 1)
        def _():
            up2.wait_recv()

        def node(h, o):
            if h == 0:
                return l0[m, 3 + j + o]
            if h == 1:
                return l1[m, 3 + x + o]
            if h == 2:
                return l2[m, 4 + x // 2 + o]
            if h == 3:
                return l3[m, lax.rem(z + o + PLANES, PLANES)]
            return l4[lax.rem(z // 2 + o + 4, 4)]

        def coupled(h):
            n = b // (1 << h)
            blocks = []
            for q, o in enumerate(OFFSETS):
                there = jnp.logical_and(n + o >= 0, n + o < (64 >> h))
                live = jnp.full((COLS, 128), far_mask[h, q, n].astype(jnp.float32)).astype(jnp.bfloat16)
                blocks.append(jnp.where(there, node(h, o), jnp.zeros((COLS, 128), jnp.bfloat16)) * live)
            return dot_nt(jnp.concatenate(blocks, axis=1), cc[m, h])

        terms = [coupled(h) for h in range(3)]

        for copy in across:
            copy.wait_recv()

        terms.append(coupled(3))
        pairs = jnp.concatenate([l3[m, 2 * i] + l3[m, 2 * i + 1] for i in range(4)], axis=0)
        lifted = lift(pairs, 3)
        for i in range(4):
            l4[i] = masked_half(lifted[i * COLS:(i + 1) * COLS], 0)
        descent = coupled(4)
        for h in (3, 2, 1, 0):
            both = dot_nn(descent.astype(jnp.bfloat16), up_t[m, h])
            side = lax.rem(b // (1 << h), 2)
            descent = terms[h] + jnp.where(side == 0, both[:, :RANK], both[:, RANK:])
        parent = descent.astype(jnp.bfloat16)
        field[...] += dot_nn(parent, trans_w[m])

        if m == 0:
            load_basis[1].wait()
            halo_recv(vec_halo)

            def join_body(g, carry):
                before = g - (g + CHUNKS - 1) // CHUNKS
                for k in range(STEP // 2):
                    coef_pair(1, vb, cpb, before * (STEP // 2) + k)
                for k in range(STEP // 2):
                    p = g * (STEP // 2) + k
                    far = far_terms(0, p)
                    for s in range(2):
                        vb[LEAF_DEV + 2 * p + s] = (near_rest(0, va, 2 * p + s) + far[s]).astype(jnp.bfloat16)

                @pl.when(jnp.logical_and(g > 0, g <= CHUNKS - HELD))
                def _():
                    start_chunk(g - 1)

                return carry

            lax.fori_loop(0, CHUNKS, join_body, 0)
            for k in range(STEP // 2):
                coef_pair(1, vb, cpb, LEAF_DEV // 2 - STEP // 2 + k)
        else:

            def final_body(p, carry):
                far = far_terms(1, p)
                total = near_acc[:, pl.ds(pl.multiple_of(p * 512, 512), 512)]
                for s in range(2):
                    where_to = pl.ds(pl.multiple_of(p * 512 + s * LEAF, LEAF), LEAF)
                    out[:, where_to] = (total[:, s * LEAF:(s + 1) * LEAF] + far[s]).astype(jnp.bfloat16)
                return carry

            lax.fori_loop(0, LEAF_DEV // 2, final_body, 0, unroll=4)

        for copy in plane + across:
            copy.wait_send()
        halo_sent(coef_halo)
        halo_sent(vec_halo)

        @pl.when(z + 1 < PLANES)
        def _():
            for copy in ups:
                copy.wait_send()

        @pl.when(z > 0)
        def _():
            for copy in downs:
                copy.wait_send()

        @pl.when(z + 2 < PLANES)
        def _():
            up2.wait_send()

        @pl.when(z > 1)
        def _():
            down2.wait_send()


def shards(
    vectors, basis, leaf_transfer, upper_transfer, upper_coupling, leaf_coupling, near_blocks,
    far_mask, far_ids, far_count, near_ids, near_count,
):
    smem = pltpu.SMEM
    i32 = jnp.int32
    hbm = pl.BlockSpec(memory_space=pltpu.HBM)
    bf = jnp.bfloat16
    f32 = jnp.float32
    dma = pltpu.SemaphoreType.DMA
    return pl.pallas_call(
        kernel,
        out_shape=jax.ShapeDtypeStruct((COLS, LEAF_DEV * LEAF), bf),
        in_specs=[hbm] * 12,
        out_specs=pl.BlockSpec(memory_space=pltpu.VMEM),
        scratch_shapes=[
            smem((5, 4, 64), i32), smem((8, LEAF_DEV), i32), smem((LEAF_DEV,), i32), smem((4, LEAF_DEV), i32), smem((LEAF_DEV,), i32),
            pltpu.VMEM((2, LEAF_DEV, 4, LEAF, LEAF), bf),
            pltpu.VMEM((2, LEAF_DEV, RANK, 512), bf),
            pltpu.VMEM((2, LEAF_DEV, RANK, LEAF), bf),
            pltpu.VMEM((2, RANK, LEAF_DEV * RANK), bf),
            pltpu.VMEM((2, 4, RANK, 128), bf),
            pltpu.VMEM((2, 5, RANK, 256), bf),
            pltpu.VMEM((97, COLS, LEAF), bf),
            pltpu.VMEM((97, COLS, LEAF), bf),
            pltpu.VMEM((COLS, 96 * RANK), bf),
            pltpu.VMEM((COLS, 96 * RANK), bf),
            pltpu.VMEM((97, COLS, 128), bf),
            pltpu.VMEM((97, COLS, 128), bf),
            pltpu.VMEM((COLS, LEAF_DEV * LEAF), f32),
            pltpu.VMEM((COLS, LEAF_DEV * RANK), f32),
            pltpu.VMEM((2, 14, COLS, 128), bf),
            pltpu.VMEM((2, 10, COLS, 128), bf),
            pltpu.VMEM((2, 10, COLS, 128), bf),
            pltpu.VMEM((2, 8, COLS, 128), bf),
            pltpu.VMEM((4, COLS, 128), bf),
            pltpu.VMEM((2, 5, RANK, 512), bf),
            dma((2, CHUNKS)), dma((9,)), dma((5,)),
            dma((2, 2)), dma((2, 2)), dma((2, 2)), dma((2, 2)),
            dma((2, 8)), dma((2, 8)), dma((2, 8)), dma((2, 8)), dma((2, 8)), dma((2, 8)),
        ],
        compiler_params=pltpu.CompilerParams(
            collective_id=0, has_side_effects=True, vmem_limit_bytes=50 << 20
        ),
        name="product",
    )(
        *(
            pltpu.with_memory_space_constraint(array, pltpu.HBM)
            for array in (
                jnp.transpose(far_mask, (0, 2, 1)), far_ids.T, far_count, near_ids.T, near_count,
                vectors, basis, leaf_transfer, upper_transfer, upper_coupling, leaf_coupling, near_blocks,
            )
        )
    )


def solution(mesh):
    return jax.shard_map(
        shards,
        mesh=mesh,
        in_specs=(
            P("col", "branch"),
            P(None, "branch", None, None),
            P(None, None, "branch"),
            P(),
            P(),
            P(None, "branch", None, None),
            P(None, "branch", None, None, None),
            P(),
            P("branch", None),
            P("branch"),
            P("branch", None),
            P("branch"),
        ),
        out_specs=P("col", "branch"),
        check_vma=False,
    )
```

```python
import jax
import jax.numpy as jnp
from jax import lax
from jax.experimental import pallas as pl
from jax.experimental.pallas import tpu as pltpu
from jax.sharding import PartitionSpec as P

OFFSETS = (-3, -2, 2, 3)
PLANE = 8
PLANES = 8
LEAF_DEV = 32
LEAF = 256
RANK = 64
COLS = 32
CHUNKS = 8
STEP = LEAF_DEV // CHUNKS
HELD = 2
EARLY = 4
AHEAD = 4
NT = (((1,), (1,)), ((), ()))
NN = (((1,), (0,)), ((), ()))


def dot_nt(a, b):
    return lax.dot_general(a, b, NT, preferred_element_type=jnp.float32)


def dot_nn(a, b):
    return lax.dot_general(a, b, NN, preferred_element_type=jnp.float32)


def kernel(
    far_mask_in, far_ids_in, far_count_in, near_ids_in, near_count_in,
    vectors, basis, leaf_transfer, upper_transfer, upper_coupling, leaf_coupling, near_blocks,
    out,
    far_mask, far_ids, far_count, near_ids, near_count,
    near_w, coup_w, basis_w, trans_w, up_t, up_c,
    va, vb, cpa, cpb, dl, dr, near_acc, field,
    l0, l1, l2, l3, l4, cc,
    sem_near, sem_in, sem_small,
    v_send, v_recv, c_send, c_recv, p_send, p_recv, z_send, z_recv, e_send, e_recv,
):
    b = lax.axis_index("branch")
    col = lax.axis_index("col")
    z = b // PLANE
    j = lax.rem(b, PLANE)
    core = lax.rem(b, 2)
    x = j // 2
    first_leaf = (b - 1) * LEAF_DEV
    lane = lax.broadcasted_iota(jnp.int32, (COLS, 128), 1)
    left = lane < 64

    def local(src, dst, sem):
        copy = pltpu.make_async_copy(src, dst, sem)
        copy.start()
        return copy

    def load_leaf(i, carry):
        local(vectors.at[:, pl.ds(pl.multiple_of(i * LEAF, LEAF), LEAF)], va.at[LEAF_DEV + i], sem_in.at[0])
        return carry

    lax.fori_loop(0, LEAF_DEV, load_leaf, 0, unroll=4)
    own = pl.ds(LEAF_DEV, LEAF_DEV)
    load_v = pltpu.make_async_copy(va.at[own], va.at[own], sem_in.at[0])
    load_basis = [None, None]
    load_trans = [None, None]
    load_coup = [None, None]
    load_near = [[], []]
    load_basis[0] = local(basis.at[0], basis_w.at[0], sem_in.at[1])
    load_trans[0] = local(leaf_transfer.at[0], trans_w.at[0], sem_in.at[2])
    load_ut = local(upper_transfer, up_t, sem_in.at[3])
    load_uc = local(upper_coupling, up_c, sem_in.at[4])
    load_small = [
        local(far_mask_in, far_mask, sem_small.at[0]),
        local(far_ids_in, far_ids, sem_small.at[1]),
        local(far_count_in, far_count, sem_small.at[2]),
        local(near_ids_in, near_ids, sem_small.at[3]),
        local(near_count_in, near_count, sem_small.at[4]),
    ]
    def start_first(m):
        if m == 1:
            load_basis[1] = local(basis.at[1], basis_w.at[1], sem_in.at[5])
            load_trans[1] = local(leaf_transfer.at[1], trans_w.at[1], sem_in.at[6])
        for g in range(2):
            part = pl.ds(g * 16, 16)
            load_near[m].append(local(near_blocks.at[m, part, 0], near_w.at[m, part, 0], sem_near.at[m, g]))
        load_coup[m] = local(leaf_coupling.at[m], coup_w.at[m], sem_in.at[7 + m])

    def start_rest(m):
        for g in range(6):
            part = pl.ds((g % 2) * 16, 16)
            slot = 1 + g // 2
            load_near[m].append(local(near_blocks.at[m, part, slot], near_w.at[m, part, slot], sem_near.at[m, 2 + g]))

    start_first(0)

    barrier = pltpu.get_barrier_semaphore()

    def greet(target):
        pl.semaphore_signal(barrier, inc=1, device_id=(target, col), device_id_type=pl.DeviceIdType.MESH)

    plane_peer = [z * PLANE + lax.rem(j + d, PLANE) for d in range(PLANE)]
    z_peer = [lax.rem(z + d, PLANES) * PLANE + j for d in range(PLANES)]

    @pl.when(b > 0)
    def _():
        greet(b - 1)

    @pl.when(b < PLANE * PLANES - 1)
    def _():
        greet(b + 1)

    for d in range(1, PLANE):
        greet(plane_peer[d])
    for d in range(1, PLANES):
        greet(z_peer[d])

    va[96] = jnp.zeros((COLS, LEAF), jnp.bfloat16)
    vb[96] = jnp.zeros((COLS, LEAF), jnp.bfloat16)
    dl[96] = jnp.zeros((COLS, 128), jnp.bfloat16)
    dr[96] = jnp.zeros((COLS, 128), jnp.bfloat16)

    def remote(src, dst, send, recv, target):
        return pltpu.make_async_remote_copy(
            src_ref=src, dst_ref=dst, send_sem=send, recv_sem=recv,
            device_id=(target, col), device_id_type=pl.DeviceIdType.MESH,
        )

    def halo_sends(m, mine, to_right, to_left, send, recv):
        return (
            remote(mine, to_right, send.at[m, 0], recv.at[m, 0], b + 1),
            remote(mine, to_left, send.at[m, 1], recv.at[m, 1], b - 1),
        )

    has_right = b < PLANE * PLANES - 1
    has_left = b > 0

    def halo_start(copies):
        @pl.when(has_right)
        def _():
            copies[0].start()

        @pl.when(has_left)
        def _():
            copies[1].start()

    def near_copies(copies, early):
        @pl.when(has_right if early else j < PLANE - 1)
        def _():
            copies[0].start()

        @pl.when(has_left if early else j > 0)
        def _():
            copies[1].start()

    def late_copies(copies):
        @pl.when(jnp.logical_and(has_right, j == PLANE - 1))
        def _():
            copies[0].start()

        @pl.when(jnp.logical_and(has_left, j == 0))
        def _():
            copies[1].start()

    def halo_recv(copies):
        @pl.when(has_left)
        def _():
            copies[0].wait_recv()

        @pl.when(has_right)
        def _():
            copies[1].wait_recv()

    def halo_sent(copies):
        @pl.when(has_right)
        def _():
            copies[0].wait_send()

        @pl.when(has_left)
        def _():
            copies[1].wait_send()

    def halves(pair):
        turned = pltpu.roll(pair, 64, 1)
        none = jnp.zeros_like(pair)
        return (
            jnp.where(left, pair, none).astype(jnp.bfloat16),
            jnp.where(left, none, turned).astype(jnp.bfloat16),
            jnp.where(left, turned, none).astype(jnp.bfloat16),
            jnp.where(left, none, pair).astype(jnp.bfloat16),
        )

    def put_halves(leaf, pair):
        al, ar, bl, br = halves(pair)
        dl[leaf] = al
        dr[leaf] = ar
        dl[leaf + 1] = bl
        dr[leaf + 1] = br

    def coef_pair(m, source, cp, p):
        lhs = source[pl.ds(LEAF_DEV + 2 * p, 2)].reshape(2 * COLS, LEAF)
        rhs = basis_w[m, pl.ds(2 * p, 2)].reshape(128, LEAF)
        both = dot_nt(lhs, rhs)
        got = jnp.where(left, both[:COLS], both[COLS:])
        cp[:, pl.ds(pl.multiple_of(LEAF_DEV * RANK + p * 128, 128), 128)] = got.astype(jnp.bfloat16)
        put_halves(LEAF_DEV + 2 * p, got)

    def masked_half(both, parity):
        keep = jnp.logical_xor(left, parity == 1)
        return jnp.where(keep, both, jnp.zeros_like(both)).astype(jnp.bfloat16)

    def live_or_zero(q, count, leaf):
        dead = lax.shift_right_arithmetic(q - count, 31) + 1
        return (leaf - first_leaf) + dead * (96 - (leaf - first_leaf))

    def far_rows(i):
        count = far_count[i]

        def spot(q):
            return live_or_zero(q, count, far_ids[q, i])

        return jnp.concatenate([dl[spot(2 * t)] + dr[spot(2 * t + 1)] for t in range(4)], axis=1)

    def near_rest(m, source, i):
        total = near_acc[:, pl.ds(pl.multiple_of(i * LEAF, LEAF), LEAF)]
        count = near_count[i]
        for q in range(1, 4):
            piece = source[live_or_zero(q, count, near_ids[q, i])]
            total = total + dot_nt(piece, near_w[m, i, q])
        return total

    def far_terms(m, p):
        pair = field[:, pl.ds(pl.multiple_of(p * 128, 128), 128)]
        none = jnp.zeros_like(pair)
        lhs = jnp.concatenate([jnp.where(left, pair, none), jnp.where(left, none, pair)], axis=0).astype(jnp.bfloat16)
        rhs = basis_w[m, pl.ds(2 * p, 2)].reshape(128, LEAF)
        both = dot_nn(lhs, rhs)
        return both[:COLS], both[COLS:]

    def chunk_copies(m, g):
        source = va if m == 0 else vb
        return halo_sends(
            m,
            source.at[pl.ds(LEAF_DEV + g * STEP, STEP)],
            source.at[pl.ds(g * STEP, STEP)],
            source.at[pl.ds(2 * LEAF_DEV + g * STEP, STEP)],
            v_send, v_recv,
        )

    def start_chunk(g):
        halo_start(chunk_copies(1, g))

    for m in range(2):
        source = va if m == 0 else vb
        cp = cpa if m == 0 else cpb
        if m == 0:
            load_v.wait()
            load_basis[0].wait()

            def coef_body(p, carry):
                coef_pair(0, va, cpa, p)
                return carry

            lax.fori_loop(0, LEAF_DEV // 2, coef_body, 0, unroll=4)
        load_trans[m].wait()
        box = dot_nt(cp[:, pl.ds(LEAF_DEV * RANK, LEAF_DEV * RANK)], trans_w[m])
        l0[m, 3 + j] = masked_half(jnp.concatenate([box, box], axis=1), core)
        if m == 0:
            last = PLANE * PLANES - 1
            pl.semaphore_wait(barrier, 14 + (b + last) // (last + 1) + (2 * last - b) // (last + 1))
        plane = []
        for d in range(1, PLANE):
            copy = remote(l0.at[m, 3 + j], l0.at[m, 3 + j], p_send.at[m, d], p_recv.at[m, d], plane_peer[d])
            copy.start()
            plane.append(copy)
        flat = LEAF_DEV * RANK
        coef_halo = halo_sends(
            m, cp.at[:, pl.ds(flat, flat)], cp.at[:, pl.ds(0, flat)], cp.at[:, pl.ds(2 * flat, flat)], c_send, c_recv
        )
        halo_start(coef_halo)
        vec_halo = halo_sends(
            m, source.at[own], source.at[pl.ds(0, LEAF_DEV)], source.at[pl.ds(2 * LEAF_DEV, LEAF_DEV)], v_send, v_recv
        )
        if m == 0:
            for g in range(CHUNKS):
                near_copies(chunk_copies(0, g), g < EARLY)
            start_rest(0)
        else:
            for g in range(CHUNKS - HELD, CHUNKS):
                start_chunk(g)

        if m == 0:
            for copy in load_small:
                copy.wait()
            load_ut.wait()
            load_uc.wait()
            for mm in range(2):
                for h in range(5):
                    blocks = []
                    for q in range(4):
                        one = up_c[mm, h, :, q * RANK:(q + 1) * RANK]
                        blocks += [one, one]
                    cc[mm, h] = jnp.concatenate(blocks, axis=1)

        for copy in load_near[m][:2]:
            copy.wait()

        def own_body(i, carry):
            near_acc[:, pl.ds(pl.multiple_of(i * LEAF, LEAF), LEAF)] = dot_nt(source[LEAF_DEV + i], near_w[m, i, 0])
            return carry

        lax.fori_loop(0, LEAF_DEV, own_body, 0, unroll=8)

        for copy in plane:
            copy.wait_recv()

        def lift(pairs, h):
            weight = up_t[m, h]
            return dot_nt(pairs, jnp.concatenate([weight, weight], axis=0))

        pairs = jnp.concatenate([l0[m, 3 + 2 * i] + l0[m, 4 + 2 * i] for i in range(4)], axis=0)
        lifted = lift(pairs, 0)
        n1 = [masked_half(lifted[i * COLS:(i + 1) * COLS], i % 2) for i in range(4)]
        for i in range(4):
            l1[m, 3 + i] = n1[i]
        lifted = lift(jnp.concatenate([n1[0] + n1[1], n1[2] + n1[3]], axis=0), 1)
        n2 = [masked_half(lifted[i * COLS:(i + 1) * COLS], i % 2) for i in range(2)]
        for i in range(2):
            l2[m, 4 + i] = n2[i]
        l3[m, z] = masked_half(lift(n2[0] + n2[1], 2), lax.rem(z, 2))

        across = [None]
        for d in range(1, PLANES):
            across.append(remote(l3.at[m, z], l3.at[m, z], z_send.at[m, d], z_recv.at[m, d], z_peer[d]))
        for d in (4, 3, 5, 2, 6, 1, 7):
            across[d].start()
        across = across[1:]
        up_one = b + PLANE
        down_one = b - PLANE
        up_two = b + 2 * PLANE
        down_two = b - 2 * PLANE

        def edge(k, src, dst, target):
            return remote(src, dst, e_send.at[m, k], e_recv.at[m, k], target)

        ups = [
            edge(0, l2.at[m, pl.ds(4, 2)], l2.at[m, pl.ds(2, 2)], up_one),
            edge(1, l1.at[m, pl.ds(4, 3)], l1.at[m, pl.ds(0, 3)], up_one),
            edge(2, l0.at[m, pl.ds(8, 3)], l0.at[m, pl.ds(0, 3)], up_one),
        ]
        downs = [
            edge(3, l2.at[m, pl.ds(4, 2)], l2.at[m, pl.ds(6, 2)], down_one),
            edge(4, l1.at[m, pl.ds(3, 3)], l1.at[m, pl.ds(7, 3)], down_one),
            edge(5, l0.at[m, pl.ds(3, 3)], l0.at[m, pl.ds(11, 3)], down_one),
        ]
        up2 = edge(6, l2.at[m, pl.ds(4, 2)], l2.at[m, pl.ds(0, 2)], up_two)
        down2 = edge(7, l2.at[m, pl.ds(4, 2)], l2.at[m, pl.ds(8, 2)], down_two)

        @pl.when(z + 1 < PLANES)
        def _():
            for copy in ups:
                copy.start()

        @pl.when(z > 0)
        def _():
            for copy in downs:
                copy.start()

        @pl.when(z + 2 < PLANES)
        def _():
            up2.start()

        @pl.when(z > 1)
        def _():
            down2.start()

        if m == 0:
            for g in range(EARLY, CHUNKS):
                late_copies(chunk_copies(0, g))
            start_first(1)
            start_rest(1)
        halo_recv(coef_halo)

        def dup_body(p, carry):
            for spot in (p, p + LEAF_DEV):
                pair = cp[:, pl.ds(pl.multiple_of(spot * 128, 128), 128)].astype(jnp.float32)
                put_halves(2 * spot, pair)
            return carry

        lax.fori_loop(0, LEAF_DEV // 2, dup_body, 0, unroll=4)
        load_coup[m].wait()

        def coup_body(p, carry):
            lhs = jnp.concatenate([far_rows(2 * p), far_rows(2 * p + 1)], axis=0)
            rhs = coup_w[m, pl.ds(2 * p, 2)].reshape(128, 512)
            both = dot_nt(lhs, rhs)
            field[:, pl.ds(pl.multiple_of(p * 128, 128), 128)] = jnp.where(left, both[:COLS], both[COLS:])
            return carry

        lax.fori_loop(0, LEAF_DEV // 2, coup_body, 0, unroll=4)

        for copy in load_near[m][2:]:
            copy.wait()
        halo_recv(vec_halo)

        def near_body(i, carry):
            near_acc[:, pl.ds(pl.multiple_of(i * LEAF, LEAF), LEAF)] = near_rest(m, source, i)
            return carry

        lax.fori_loop(0, AHEAD * STEP if m == 0 else LEAF_DEV, near_body, 0, unroll=4)

        @pl.when(z + 1 < PLANES)
        def _():
            for copy in downs:
                copy.wait_recv()

        @pl.when(z > 0)
        def _():
            for copy in ups:
                copy.wait_recv()

        @pl.when(z + 2 < PLANES)
        def _():
            down2.wait_recv()

        @pl.when(z > 1)
        def _():
            up2.wait_recv()

        def node(h, o):
            if h == 0:
                return l0[m, 3 + j + o]
            if h == 1:
                return l1[m, 3 + x + o]
            if h == 2:
                return l2[m, 4 + x // 2 + o]
            if h == 3:
                return l3[m, lax.rem(z + o + PLANES, PLANES)]
            return l4[lax.rem(z // 2 + o + 4, 4)]

        def coupled(h):
            n = b // (1 << h)
            blocks = []
            for q, o in enumerate(OFFSETS):
                there = jnp.logical_and(n + o >= 0, n + o < (64 >> h))
                live = jnp.full((COLS, 128), far_mask[h, q, n].astype(jnp.float32)).astype(jnp.bfloat16)
                blocks.append(jnp.where(there, node(h, o), jnp.zeros((COLS, 128), jnp.bfloat16)) * live)
            return dot_nt(jnp.concatenate(blocks, axis=1), cc[m, h])

        terms = [coupled(h) for h in range(3)]

        for copy in across:
            copy.wait_recv()

        terms.append(coupled(3))
        pairs = jnp.concatenate([l3[m, 2 * i] + l3[m, 2 * i + 1] for i in range(4)], axis=0)
        lifted = lift(pairs, 3)
        for i in range(4):
            l4[i] = masked_half(lifted[i * COLS:(i + 1) * COLS], 0)
        descent = coupled(4)
        for h in (3, 2, 1, 0):
            both = dot_nn(descent.astype(jnp.bfloat16), up_t[m, h])
            side = lax.rem(b // (1 << h), 2)
            descent = terms[h] + jnp.where(side == 0, both[:, :RANK], both[:, RANK:])
        parent = descent.astype(jnp.bfloat16)
        field[...] += dot_nn(parent, trans_w[m])

        if m == 0:
            load_basis[1].wait()

            def coef_chunk(g):
                for k in range(STEP // 2):
                    coef_pair(1, vb, cpb, g * (STEP // 2) + k)

            def join(g, near):
                for k in range(STEP // 2):
                    p = g * (STEP // 2) + k
                    far = far_terms(0, p)
                    for s in range(2):
                        i = 2 * p + s
                        total = near_rest(0, va, i) if near else near_acc[:, pl.ds(pl.multiple_of(i * LEAF, LEAF), LEAF)]
                        vb[LEAF_DEV + i] = (total + far[s]).astype(jnp.bfloat16)

            def ready_body(g, carry):
                coef_chunk(g - (g + CHUNKS - 1) // CHUNKS)
                join(g, False)

                @pl.when(g > 0)
                def _():
                    start_chunk(g - 1)

                return carry

            def join_body(g, carry):
                coef_chunk(AHEAD + g - 1)
                join(AHEAD + g, True)

                @pl.when(AHEAD + g <= CHUNKS - HELD)
                def _():
                    start_chunk(AHEAD + g - 1)

                return carry

            lax.fori_loop(0, AHEAD, ready_body, 0)
            lax.fori_loop(0, CHUNKS - AHEAD, join_body, 0)
            coef_chunk(CHUNKS - 1)
        else:

            def final_body(p, carry):
                far = far_terms(1, p)
                total = near_acc[:, pl.ds(pl.multiple_of(p * 512, 512), 512)]
                for s in range(2):
                    where_to = pl.ds(pl.multiple_of(p * 512 + s * LEAF, LEAF), LEAF)
                    out[:, where_to] = (total[:, s * LEAF:(s + 1) * LEAF] + far[s]).astype(jnp.bfloat16)
                return carry

            lax.fori_loop(0, LEAF_DEV // 2, final_body, 0, unroll=4)

        for copy in plane + across:
            copy.wait_send()
        halo_sent(coef_halo)
        halo_sent(vec_halo)

        @pl.when(z + 1 < PLANES)
        def _():
            for copy in ups:
                copy.wait_send()

        @pl.when(z > 0)
        def _():
            for copy in downs:
                copy.wait_send()

        @pl.when(z + 2 < PLANES)
        def _():
            up2.wait_send()

        @pl.when(z > 1)
        def _():
            down2.wait_send()


def shards(
    vectors, basis, leaf_transfer, upper_transfer, upper_coupling, leaf_coupling, near_blocks,
    far_mask, far_ids, far_count, near_ids, near_count,
):
    smem = pltpu.SMEM
    i32 = jnp.int32
    hbm = pl.BlockSpec(memory_space=pltpu.HBM)
    bf = jnp.bfloat16
    f32 = jnp.float32
    dma = pltpu.SemaphoreType.DMA
    return pl.pallas_call(
        kernel,
        out_shape=jax.ShapeDtypeStruct((COLS, LEAF_DEV * LEAF), bf),
        in_specs=[hbm] * 12,
        out_specs=pl.BlockSpec(memory_space=pltpu.VMEM),
        scratch_shapes=[
            smem((5, 4, 64), i32), smem((8, LEAF_DEV), i32), smem((LEAF_DEV,), i32), smem((4, LEAF_DEV), i32), smem((LEAF_DEV,), i32),
            pltpu.VMEM((2, LEAF_DEV, 4, LEAF, LEAF), bf),
            pltpu.VMEM((2, LEAF_DEV, RANK, 512), bf),
            pltpu.VMEM((2, LEAF_DEV, RANK, LEAF), bf),
            pltpu.VMEM((2, RANK, LEAF_DEV * RANK), bf),
            pltpu.VMEM((2, 4, RANK, 128), bf),
            pltpu.VMEM((2, 5, RANK, 256), bf),
            pltpu.VMEM((97, COLS, LEAF), bf),
            pltpu.VMEM((97, COLS, LEAF), bf),
            pltpu.VMEM((COLS, 96 * RANK), bf),
            pltpu.VMEM((COLS, 96 * RANK), bf),
            pltpu.VMEM((97, COLS, 128), bf),
            pltpu.VMEM((97, COLS, 128), bf),
            pltpu.VMEM((COLS, LEAF_DEV * LEAF), f32),
            pltpu.VMEM((COLS, LEAF_DEV * RANK), f32),
            pltpu.VMEM((2, 14, COLS, 128), bf),
            pltpu.VMEM((2, 10, COLS, 128), bf),
            pltpu.VMEM((2, 10, COLS, 128), bf),
            pltpu.VMEM((2, 8, COLS, 128), bf),
            pltpu.VMEM((4, COLS, 128), bf),
            pltpu.VMEM((2, 5, RANK, 512), bf),
            dma((2, CHUNKS)), dma((9,)), dma((5,)),
            dma((2, 2)), dma((2, 2)), dma((2, 2)), dma((2, 2)),
            dma((2, 8)), dma((2, 8)), dma((2, 8)), dma((2, 8)), dma((2, 8)), dma((2, 8)),
        ],
        compiler_params=pltpu.CompilerParams(
            collective_id=0, has_side_effects=True, vmem_limit_bytes=50 << 20
        ),
        name="product",
    )(
        *(
            pltpu.with_memory_space_constraint(array, pltpu.HBM)
            for array in (
                jnp.transpose(far_mask, (0, 2, 1)), far_ids.T, far_count, near_ids.T, near_count,
                vectors, basis, leaf_transfer, upper_transfer, upper_coupling, leaf_coupling, near_blocks,
            )
        )
    )


def solution(mesh):
    return jax.shard_map(
        shards,
        mesh=mesh,
        in_specs=(
            P("col", "branch"),
            P(None, "branch", None, None),
            P(None, None, "branch"),
            P(),
            P(),
            P(None, "branch", None, None),
            P(None, "branch", None, None, None),
            P(),
            P("branch", None),
            P("branch"),
            P("branch", None),
            P("branch"),
        ),
        out_specs=P("col", "branch"),
        check_vma=False,
    )
```

```python
import jax
import jax.numpy as jnp
from jax import lax
from jax.experimental import pallas as pl
from jax.experimental.pallas import tpu as pltpu
from jax.sharding import PartitionSpec as P

OFFSETS = (-3, -2, 2, 3)
PLANE = 8
PLANES = 8
LEAF_DEV = 32
LEAF = 256
RANK = 64
COLS = 32
CHUNKS = 8
STEP = LEAF_DEV // CHUNKS
HELD = 2
EARLY = 8
AHEAD = 2
NT = (((1,), (1,)), ((), ()))
NN = (((1,), (0,)), ((), ()))


def dot_nt(a, b):
    return lax.dot_general(a, b, NT, preferred_element_type=jnp.float32)


def dot_nn(a, b):
    return lax.dot_general(a, b, NN, preferred_element_type=jnp.float32)


def kernel(
    far_mask_in, far_ids_in, far_count_in, near_ids_in, near_count_in,
    vectors, basis, leaf_transfer, upper_transfer, upper_coupling, leaf_coupling, near_blocks,
    out,
    far_mask, far_ids, far_count, near_ids, near_count,
    near_w, coup_w, basis_w, trans_w, up_t, up_c,
    va, vb, cpa, cpb, dl, dr, near_acc, field,
    l0, l1, l2, l3, l4, cc, down_w,
    sem_near, sem_in, sem_small,
    v_send, v_recv, c_send, c_recv, p_send, p_recv, z_send, z_recv, e_send, e_recv,
):
    b = lax.axis_index("branch")
    col = lax.axis_index("col")
    z = b // PLANE
    j = lax.rem(b, PLANE)
    core = lax.rem(b, 2)
    x = j // 2
    first_leaf = (b - 1) * LEAF_DEV
    lane = lax.broadcasted_iota(jnp.int32, (COLS, 128), 1)
    left = lane < 64

    def local(src, dst, sem):
        copy = pltpu.make_async_copy(src, dst, sem)
        copy.start()
        return copy

    def load_leaf(i, carry):
        local(vectors.at[:, pl.ds(pl.multiple_of(i * LEAF, LEAF), LEAF)], va.at[LEAF_DEV + i], sem_in.at[0])
        return carry

    lax.fori_loop(0, LEAF_DEV, load_leaf, 0, unroll=4)
    own = pl.ds(LEAF_DEV, LEAF_DEV)
    load_v = pltpu.make_async_copy(va.at[own], va.at[own], sem_in.at[0])
    load_basis = [None, None]
    load_trans = [None, None]
    load_coup = [None, None]
    load_near = [[], []]
    load_basis[0] = local(basis.at[0], basis_w.at[0], sem_in.at[1])
    load_trans[0] = local(leaf_transfer.at[0], trans_w.at[0], sem_in.at[2])
    load_ut = local(upper_transfer, up_t, sem_in.at[3])
    load_uc = local(upper_coupling, up_c, sem_in.at[4])
    load_small = [
        local(far_mask_in, far_mask, sem_small.at[0]),
        local(far_ids_in, far_ids, sem_small.at[1]),
        local(far_count_in, far_count, sem_small.at[2]),
        local(near_ids_in, near_ids, sem_small.at[3]),
        local(near_count_in, near_count, sem_small.at[4]),
    ]
    def start_first(m):
        if m == 1:
            load_basis[1] = local(basis.at[1], basis_w.at[1], sem_in.at[5])
            load_trans[1] = local(leaf_transfer.at[1], trans_w.at[1], sem_in.at[6])
        for g in range(2):
            part = pl.ds(g * 16, 16)
            load_near[m].append(local(near_blocks.at[m, part, 0], near_w.at[m, part, 0], sem_near.at[m, g]))
        load_coup[m] = local(leaf_coupling.at[m], coup_w.at[m], sem_in.at[7 + m])

    def start_rest(m):
        for g in range(6):
            part = pl.ds((g % 2) * 16, 16)
            slot = 1 + g // 2
            load_near[m].append(local(near_blocks.at[m, part, slot], near_w.at[m, part, slot], sem_near.at[m, 2 + g]))

    start_first(0)

    barrier = pltpu.get_barrier_semaphore()

    def greet(target):
        pl.semaphore_signal(barrier, inc=1, device_id=(target, col), device_id_type=pl.DeviceIdType.MESH)

    plane_peer = [z * PLANE + lax.rem(j + d, PLANE) for d in range(PLANE)]
    z_peer = [lax.rem(z + d, PLANES) * PLANE + j for d in range(PLANES)]

    @pl.when(b > 0)
    def _():
        greet(b - 1)

    @pl.when(b < PLANE * PLANES - 1)
    def _():
        greet(b + 1)

    for d in range(1, PLANE):
        greet(plane_peer[d])
    for d in range(1, PLANES):
        greet(z_peer[d])

    va[96] = jnp.zeros((COLS, LEAF), jnp.bfloat16)
    vb[96] = jnp.zeros((COLS, LEAF), jnp.bfloat16)
    dl[96] = jnp.zeros((COLS, 128), jnp.bfloat16)
    dr[96] = jnp.zeros((COLS, 128), jnp.bfloat16)

    def remote(src, dst, send, recv, target):
        return pltpu.make_async_remote_copy(
            src_ref=src, dst_ref=dst, send_sem=send, recv_sem=recv,
            device_id=(target, col), device_id_type=pl.DeviceIdType.MESH,
        )

    def halo_sends(m, mine, to_right, to_left, send, recv):
        return (
            remote(mine, to_right, send.at[m, 0], recv.at[m, 0], b + 1),
            remote(mine, to_left, send.at[m, 1], recv.at[m, 1], b - 1),
        )

    has_right = b < PLANE * PLANES - 1
    has_left = b > 0

    def halo_start(copies):
        @pl.when(has_right)
        def _():
            copies[0].start()

        @pl.when(has_left)
        def _():
            copies[1].start()

    def near_copies(copies, early):
        @pl.when(has_right if early else j < PLANE - 1)
        def _():
            copies[0].start()

        @pl.when(has_left if early else j > 0)
        def _():
            copies[1].start()

    def late_copies(copies):
        @pl.when(jnp.logical_and(has_right, j == PLANE - 1))
        def _():
            copies[0].start()

        @pl.when(jnp.logical_and(has_left, j == 0))
        def _():
            copies[1].start()

    def halo_recv(copies):
        @pl.when(has_left)
        def _():
            copies[0].wait_recv()

        @pl.when(has_right)
        def _():
            copies[1].wait_recv()

    def halo_sent(copies):
        @pl.when(has_right)
        def _():
            copies[0].wait_send()

        @pl.when(has_left)
        def _():
            copies[1].wait_send()

    def halves(pair):
        turned = pltpu.roll(pair, 64, 1)
        none = jnp.zeros_like(pair)
        return (
            jnp.where(left, pair, none).astype(jnp.bfloat16),
            jnp.where(left, none, turned).astype(jnp.bfloat16),
            jnp.where(left, turned, none).astype(jnp.bfloat16),
            jnp.where(left, none, pair).astype(jnp.bfloat16),
        )

    def put_halves(leaf, pair):
        al, ar, bl, br = halves(pair)
        dl[leaf] = al
        dr[leaf] = ar
        dl[leaf + 1] = bl
        dr[leaf + 1] = br

    def coef_pair(m, source, cp, p):
        lhs = source[pl.ds(LEAF_DEV + 2 * p, 2)].reshape(2 * COLS, LEAF)
        rhs = basis_w[m, pl.ds(2 * p, 2)].reshape(128, LEAF)
        both = dot_nt(lhs, rhs)
        got = jnp.where(left, both[:COLS], both[COLS:])
        cp[:, pl.ds(pl.multiple_of(LEAF_DEV * RANK + p * 128, 128), 128)] = got.astype(jnp.bfloat16)
        put_halves(LEAF_DEV + 2 * p, got)

    def masked_half(both, parity):
        keep = jnp.logical_xor(left, parity == 1)
        return jnp.where(keep, both, jnp.zeros_like(both)).astype(jnp.bfloat16)

    def live_or_zero(q, count, leaf):
        dead = lax.shift_right_arithmetic(q - count, 31) + 1
        return (leaf - first_leaf) + dead * (96 - (leaf - first_leaf))

    def far_rows(i):
        count = far_count[i]

        def spot(q):
            return live_or_zero(q, count, far_ids[q, i])

        return jnp.concatenate([dl[spot(2 * t)] + dr[spot(2 * t + 1)] for t in range(4)], axis=1)

    def near_rest(m, source, i):
        total = near_acc[:, pl.ds(pl.multiple_of(i * LEAF, LEAF), LEAF)]
        count = near_count[i]
        for q in range(1, 4):
            piece = source[live_or_zero(q, count, near_ids[q, i])]
            total = total + dot_nt(piece, near_w[m, i, q])
        return total

    def far_terms(m, p):
        pair = field[:, pl.ds(pl.multiple_of(p * 128, 128), 128)]
        none = jnp.zeros_like(pair)
        lhs = jnp.concatenate([jnp.where(left, pair, none), jnp.where(left, none, pair)], axis=0).astype(jnp.bfloat16)
        rhs = basis_w[m, pl.ds(2 * p, 2)].reshape(128, LEAF)
        both = dot_nn(lhs, rhs)
        return both[:COLS], both[COLS:]

    def chunk_copies(m, g):
        source = va if m == 0 else vb
        return halo_sends(
            m,
            source.at[pl.ds(LEAF_DEV + g * STEP, STEP)],
            source.at[pl.ds(g * STEP, STEP)],
            source.at[pl.ds(2 * LEAF_DEV + g * STEP, STEP)],
            v_send, v_recv,
        )

    def start_chunk(g):
        halo_start(chunk_copies(1, g))

    for m in range(2):
        source = va if m == 0 else vb
        cp = cpa if m == 0 else cpb
        if m == 0:
            load_v.wait()
            load_basis[0].wait()

            def coef_body(p, carry):
                coef_pair(0, va, cpa, p)
                return carry

            lax.fori_loop(0, LEAF_DEV // 2, coef_body, 0, unroll=4)
        load_trans[m].wait()
        box = dot_nt(cp[:, pl.ds(LEAF_DEV * RANK, LEAF_DEV * RANK)], trans_w[m])
        l0[m, 3 + j] = masked_half(jnp.concatenate([box, box], axis=1), core)
        if m == 0:
            last = PLANE * PLANES - 1
            pl.semaphore_wait(barrier, 14 + (b + last) // (last + 1) + (2 * last - b) // (last + 1))
        plane = []
        for d in range(1, PLANE):
            copy = remote(l0.at[m, 3 + j], l0.at[m, 3 + j], p_send.at[m, d], p_recv.at[m, d], plane_peer[d])
            copy.start()
            plane.append(copy)
        flat = LEAF_DEV * RANK
        coef_halo = halo_sends(
            m, cp.at[:, pl.ds(flat, flat)], cp.at[:, pl.ds(0, flat)], cp.at[:, pl.ds(2 * flat, flat)], c_send, c_recv
        )
        halo_start(coef_halo)
        vec_halo = halo_sends(
            m, source.at[own], source.at[pl.ds(0, LEAF_DEV)], source.at[pl.ds(2 * LEAF_DEV, LEAF_DEV)], v_send, v_recv
        )
        if m == 0:
            for g in range(CHUNKS):
                near_copies(chunk_copies(0, g), g < EARLY)
            start_rest(0)
        else:
            for g in range(CHUNKS - HELD, CHUNKS):
                start_chunk(g)

        if m == 0:
            for copy in load_small:
                copy.wait()
            load_ut.wait()
            load_uc.wait()
            for mm in range(2):
                for h in range(5):
                    blocks = []
                    for q in range(4):
                        one = up_c[mm, h, :, q * RANK:(q + 1) * RANK]
                        blocks += [one, one]
                    cc[mm, h] = jnp.concatenate(blocks, axis=1)
                chain = None
                for h in range(4):
                    half = jnp.where(lax.rem(b // (1 << h), 2) == 0, up_t[mm, h, :, :RANK], up_t[mm, h, :, RANK:])
                    chain = half if chain is None else dot_nn(half, chain).astype(jnp.bfloat16)
                    down_w[mm, h] = chain

        for copy in load_near[m][:2]:
            copy.wait()

        def own_body(i, carry):
            near_acc[:, pl.ds(pl.multiple_of(i * LEAF, LEAF), LEAF)] = dot_nt(source[LEAF_DEV + i], near_w[m, i, 0])
            return carry

        lax.fori_loop(0, LEAF_DEV, own_body, 0, unroll=8)

        for copy in plane:
            copy.wait_recv()

        def lift(pairs, h):
            weight = up_t[m, h]
            return dot_nt(pairs, jnp.concatenate([weight, weight], axis=0))

        pairs = jnp.concatenate([l0[m, 3 + 2 * i] + l0[m, 4 + 2 * i] for i in range(4)], axis=0)
        lifted = lift(pairs, 0)
        n1 = [masked_half(lifted[i * COLS:(i + 1) * COLS], i % 2) for i in range(4)]
        for i in range(4):
            l1[m, 3 + i] = n1[i]
        lifted = lift(jnp.concatenate([n1[0] + n1[1], n1[2] + n1[3]], axis=0), 1)
        n2 = [masked_half(lifted[i * COLS:(i + 1) * COLS], i % 2) for i in range(2)]
        for i in range(2):
            l2[m, 4 + i] = n2[i]
        l3[m, z] = masked_half(lift(n2[0] + n2[1], 2), lax.rem(z, 2))

        across = [None]
        for d in range(1, PLANES):
            across.append(remote(l3.at[m, z], l3.at[m, z], z_send.at[m, d], z_recv.at[m, d], z_peer[d]))
        for d in (4, 3, 5, 2, 6, 1, 7):
            across[d].start()
        across = across[1:]
        up_one = b + PLANE
        down_one = b - PLANE
        up_two = b + 2 * PLANE
        down_two = b - 2 * PLANE

        def edge(k, src, dst, target):
            return remote(src, dst, e_send.at[m, k], e_recv.at[m, k], target)

        ups = [
            edge(0, l2.at[m, pl.ds(4, 2)], l2.at[m, pl.ds(2, 2)], up_one),
            edge(1, l1.at[m, pl.ds(4, 3)], l1.at[m, pl.ds(0, 3)], up_one),
            edge(2, l0.at[m, pl.ds(8, 3)], l0.at[m, pl.ds(0, 3)], up_one),
        ]
        downs = [
            edge(3, l2.at[m, pl.ds(4, 2)], l2.at[m, pl.ds(6, 2)], down_one),
            edge(4, l1.at[m, pl.ds(3, 3)], l1.at[m, pl.ds(7, 3)], down_one),
            edge(5, l0.at[m, pl.ds(3, 3)], l0.at[m, pl.ds(11, 3)], down_one),
        ]
        up2 = edge(6, l2.at[m, pl.ds(4, 2)], l2.at[m, pl.ds(0, 2)], up_two)
        down2 = edge(7, l2.at[m, pl.ds(4, 2)], l2.at[m, pl.ds(8, 2)], down_two)

        @pl.when(z + 1 < PLANES)
        def _():
            for copy in ups:
                copy.start()

        @pl.when(z > 0)
        def _():
            for copy in downs:
                copy.start()

        @pl.when(z + 2 < PLANES)
        def _():
            up2.start()

        @pl.when(z > 1)
        def _():
            down2.start()

        if m == 0:
            for g in range(EARLY, CHUNKS):
                late_copies(chunk_copies(0, g))
            start_first(1)
            start_rest(1)
        halo_recv(coef_halo)

        def dup_body(p, carry):
            for spot in (p, p + LEAF_DEV):
                pair = cp[:, pl.ds(pl.multiple_of(spot * 128, 128), 128)].astype(jnp.float32)
                put_halves(2 * spot, pair)
            return carry

        lax.fori_loop(0, LEAF_DEV // 2, dup_body, 0, unroll=4)
        load_coup[m].wait()

        def coup_body(p, carry):
            lhs = jnp.concatenate([far_rows(2 * p), far_rows(2 * p + 1)], axis=0)
            rhs = coup_w[m, pl.ds(2 * p, 2)].reshape(128, 512)
            both = dot_nt(lhs, rhs)
            field[:, pl.ds(pl.multiple_of(p * 128, 128), 128)] = jnp.where(left, both[:COLS], both[COLS:])
            return carry

        lax.fori_loop(0, LEAF_DEV // 2, coup_body, 0, unroll=8)

        for copy in load_near[m][2:]:
            copy.wait()
        halo_recv(vec_halo)

        def near_body(i, carry):
            near_acc[:, pl.ds(pl.multiple_of(i * LEAF, LEAF), LEAF)] = near_rest(m, source, i)
            return carry

        lax.fori_loop(0, AHEAD * STEP if m == 0 else LEAF_DEV, near_body, 0, unroll=8)

        @pl.when(z + 1 < PLANES)
        def _():
            for copy in downs:
                copy.wait_recv()

        @pl.when(z > 0)
        def _():
            for copy in ups:
                copy.wait_recv()

        @pl.when(z + 2 < PLANES)
        def _():
            down2.wait_recv()

        @pl.when(z > 1)
        def _():
            up2.wait_recv()

        def node(h, o):
            if h == 0:
                return l0[m, 3 + j + o]
            if h == 1:
                return l1[m, 3 + x + o]
            if h == 2:
                return l2[m, 4 + x // 2 + o]
            if h == 3:
                return l3[m, lax.rem(z + o + PLANES, PLANES)]
            return l4[lax.rem(z // 2 + o + 4, 4)]

        def coupled(h):
            n = b // (1 << h)
            blocks = []
            for q, o in enumerate(OFFSETS):
                there = jnp.logical_and(n + o >= 0, n + o < (64 >> h))
                live = jnp.full((COLS, 128), far_mask[h, q, n].astype(jnp.float32)).astype(jnp.bfloat16)
                blocks.append(jnp.where(there, node(h, o), jnp.zeros((COLS, 128), jnp.bfloat16)) * live)
            return dot_nt(jnp.concatenate(blocks, axis=1), cc[m, h])

        def brought(h, term):
            return dot_nn(term.astype(jnp.bfloat16), down_w[m, h - 1])

        descent = coupled(0) + brought(1, coupled(1)) + brought(2, coupled(2))

        for copy in across:
            copy.wait_recv()

        descent = descent + brought(3, coupled(3))
        pairs = jnp.concatenate([l3[m, 2 * i] + l3[m, 2 * i + 1] for i in range(4)], axis=0)
        lifted = lift(pairs, 3)
        for i in range(4):
            l4[i] = masked_half(lifted[i * COLS:(i + 1) * COLS], 0)
        descent = descent + brought(4, coupled(4))
        parent = descent.astype(jnp.bfloat16)
        field[...] += dot_nn(parent, trans_w[m])

        if m == 0:
            load_basis[1].wait()

            def coef_chunk(g):
                for k in range(STEP // 2):
                    coef_pair(1, vb, cpb, g * (STEP // 2) + k)

            def join(g, near):
                for k in range(STEP // 2):
                    p = g * (STEP // 2) + k
                    far = far_terms(0, p)
                    for s in range(2):
                        i = 2 * p + s
                        total = near_rest(0, va, i) if near else near_acc[:, pl.ds(pl.multiple_of(i * LEAF, LEAF), LEAF)]
                        vb[LEAF_DEV + i] = (total + far[s]).astype(jnp.bfloat16)

            def ready_body(g, carry):
                coef_chunk(g - (g + CHUNKS - 1) // CHUNKS)
                join(g, False)

                @pl.when(g > 0)
                def _():
                    start_chunk(g - 1)

                return carry

            def join_body(g, carry):
                coef_chunk(AHEAD + g - 1)
                join(AHEAD + g, True)

                @pl.when(AHEAD + g <= CHUNKS - HELD)
                def _():
                    start_chunk(AHEAD + g - 1)

                return carry

            lax.fori_loop(0, AHEAD, ready_body, 0)
            lax.fori_loop(0, CHUNKS - AHEAD, join_body, 0)
            coef_chunk(CHUNKS - 1)
        else:

            def final_body(p, carry):
                far = far_terms(1, p)
                total = near_acc[:, pl.ds(pl.multiple_of(p * 512, 512), 512)]
                for s in range(2):
                    where_to = pl.ds(pl.multiple_of(p * 512 + s * LEAF, LEAF), LEAF)
                    out[:, where_to] = (total[:, s * LEAF:(s + 1) * LEAF] + far[s]).astype(jnp.bfloat16)
                return carry

            lax.fori_loop(0, LEAF_DEV // 2, final_body, 0, unroll=4)

        for copy in plane + across:
            copy.wait_send()
        halo_sent(coef_halo)
        halo_sent(vec_halo)

        @pl.when(z + 1 < PLANES)
        def _():
            for copy in ups:
                copy.wait_send()

        @pl.when(z > 0)
        def _():
            for copy in downs:
                copy.wait_send()

        @pl.when(z + 2 < PLANES)
        def _():
            up2.wait_send()

        @pl.when(z > 1)
        def _():
            down2.wait_send()


def shards(
    vectors, basis, leaf_transfer, upper_transfer, upper_coupling, leaf_coupling, near_blocks,
    far_mask, far_ids, far_count, near_ids, near_count,
):
    smem = pltpu.SMEM
    i32 = jnp.int32
    hbm = pl.BlockSpec(memory_space=pltpu.HBM)
    bf = jnp.bfloat16
    f32 = jnp.float32
    dma = pltpu.SemaphoreType.DMA
    return pl.pallas_call(
        kernel,
        out_shape=jax.ShapeDtypeStruct((COLS, LEAF_DEV * LEAF), bf),
        in_specs=[hbm] * 12,
        out_specs=pl.BlockSpec(memory_space=pltpu.VMEM),
        scratch_shapes=[
            smem((5, 4, 64), i32), smem((8, LEAF_DEV), i32), smem((LEAF_DEV,), i32), smem((4, LEAF_DEV), i32), smem((LEAF_DEV,), i32),
            pltpu.VMEM((2, LEAF_DEV, 4, LEAF, LEAF), bf),
            pltpu.VMEM((2, LEAF_DEV, RANK, 512), bf),
            pltpu.VMEM((2, LEAF_DEV, RANK, LEAF), bf),
            pltpu.VMEM((2, RANK, LEAF_DEV * RANK), bf),
            pltpu.VMEM((2, 4, RANK, 128), bf),
            pltpu.VMEM((2, 5, RANK, 256), bf),
            pltpu.VMEM((97, COLS, LEAF), bf),
            pltpu.VMEM((97, COLS, LEAF), bf),
            pltpu.VMEM((COLS, 96 * RANK), bf),
            pltpu.VMEM((COLS, 96 * RANK), bf),
            pltpu.VMEM((97, COLS, 128), bf),
            pltpu.VMEM((97, COLS, 128), bf),
            pltpu.VMEM((COLS, LEAF_DEV * LEAF), f32),
            pltpu.VMEM((COLS, LEAF_DEV * RANK), f32),
            pltpu.VMEM((2, 14, COLS, 128), bf),
            pltpu.VMEM((2, 10, COLS, 128), bf),
            pltpu.VMEM((2, 10, COLS, 128), bf),
            pltpu.VMEM((2, 8, COLS, 128), bf),
            pltpu.VMEM((4, COLS, 128), bf),
            pltpu.VMEM((2, 5, RANK, 512), bf),
            pltpu.VMEM((2, 4, RANK, RANK), bf),
            dma((2, CHUNKS)), dma((9,)), dma((5,)),
            dma((2, 2)), dma((2, 2)), dma((2, 2)), dma((2, 2)),
            dma((2, 8)), dma((2, 8)), dma((2, 8)), dma((2, 8)), dma((2, 8)), dma((2, 8)),
        ],
        compiler_params=pltpu.CompilerParams(
            collective_id=0, has_side_effects=True, vmem_limit_bytes=50 << 20
        ),
        name="product",
    )(
        *(
            pltpu.with_memory_space_constraint(array, pltpu.HBM)
            for array in (
                jnp.transpose(far_mask, (0, 2, 1)), far_ids.T, far_count, near_ids.T, near_count,
                vectors, basis, leaf_transfer, upper_transfer, upper_coupling, leaf_coupling, near_blocks,
            )
        )
    )


def solution(mesh):
    return jax.shard_map(
        shards,
        mesh=mesh,
        in_specs=(
            P("col", "branch"),
            P(None, "branch", None, None),
            P(None, None, "branch"),
            P(),
            P(),
            P(None, "branch", None, None),
            P(None, "branch", None, None, None),
            P(),
            P("branch", None),
            P("branch"),
            P("branch", None),
            P("branch"),
        ),
        out_specs=P("col", "branch"),
        check_vma=False,
    )
```

```python
import jax
import jax.numpy as jnp
from jax import lax
from jax.experimental import pallas as pl
from jax.experimental.pallas import tpu as pltpu
from jax.sharding import PartitionSpec as P

OFFSETS = (-3, -2, 2, 3)
PLANE = 8
PLANES = 8
LEAF_DEV = 32
LEAF = 256
RANK = 64
COLS = 32
CHUNKS = 8
STEP = LEAF_DEV // CHUNKS
HELD = 2
EARLY = 8
AHEAD = 2
NT = (((1,), (1,)), ((), ()))
NN = (((1,), (0,)), ((), ()))


def dot_nt(a, b):
    return lax.dot_general(a, b, NT, preferred_element_type=jnp.float32)


def dot_nn(a, b):
    return lax.dot_general(a, b, NN, preferred_element_type=jnp.float32)


def kernel(
    far_mask_in, far_ids_in, far_count_in, near_ids_in, near_count_in,
    vectors, basis, leaf_transfer, upper_transfer, upper_coupling, leaf_coupling, near_blocks,
    out,
    far_mask, far_ids, far_count, near_ids, near_count,
    near_w, coup_w, basis_w, trans_w, up_t, up_c,
    va, vb, cpa, cpb, dl, dr, near_acc, field,
    l0, l1, l2, l3, l4, cc, down_w,
    sem_near, sem_in, sem_small,
    v_send, v_recv, c_send, c_recv, p_send, p_recv, z_send, z_recv, e_send, e_recv,
):
    b = lax.axis_index("branch")
    col = lax.axis_index("col")
    z = b // PLANE
    j = lax.rem(b, PLANE)
    core = lax.rem(b, 2)
    x = j // 2
    first_leaf = (b - 1) * LEAF_DEV
    lane = lax.broadcasted_iota(jnp.int32, (COLS, 128), 1)
    left = lane < 64

    def local(src, dst, sem):
        copy = pltpu.make_async_copy(src, dst, sem)
        copy.start()
        return copy

    def load_leaf(i, carry):
        local(vectors.at[:, pl.ds(pl.multiple_of(i * LEAF, LEAF), LEAF)], va.at[LEAF_DEV + i], sem_in.at[0])
        return carry

    lax.fori_loop(0, LEAF_DEV, load_leaf, 0, unroll=4)
    own = pl.ds(LEAF_DEV, LEAF_DEV)
    load_v = pltpu.make_async_copy(va.at[own], va.at[own], sem_in.at[0])
    load_basis = [None, None]
    load_trans = [None, None]
    load_coup = [None, None]
    load_near = [[], []]
    load_basis[0] = local(basis.at[0], basis_w.at[0], sem_in.at[1])
    load_trans[0] = local(leaf_transfer.at[0], trans_w.at[0], sem_in.at[2])
    load_ut = local(upper_transfer, up_t, sem_in.at[3])
    load_uc = local(upper_coupling, up_c, sem_in.at[4])
    load_small = [
        local(far_mask_in, far_mask, sem_small.at[0]),
        local(far_ids_in, far_ids, sem_small.at[1]),
        local(far_count_in, far_count, sem_small.at[2]),
        local(near_ids_in, near_ids, sem_small.at[3]),
        local(near_count_in, near_count, sem_small.at[4]),
    ]
    def start_first(m):
        if m == 1:
            load_basis[1] = local(basis.at[1], basis_w.at[1], sem_in.at[5])
            load_trans[1] = local(leaf_transfer.at[1], trans_w.at[1], sem_in.at[6])
        for g in range(2):
            part = pl.ds(g * 16, 16)
            load_near[m].append(local(near_blocks.at[m, part, 0], near_w.at[m, part, 0], sem_near.at[m, g]))
        load_coup[m] = local(leaf_coupling.at[m], coup_w.at[m], sem_in.at[7 + m])

    def start_rest(m):
        for g in range(6):
            part = pl.ds((g % 2) * 16, 16)
            slot = 1 + g // 2
            load_near[m].append(local(near_blocks.at[m, part, slot], near_w.at[m, part, slot], sem_near.at[m, 2 + g]))

    start_first(0)

    barrier = pltpu.get_barrier_semaphore()

    def greet(target):
        pl.semaphore_signal(barrier, inc=1, device_id=(target, col), device_id_type=pl.DeviceIdType.MESH)

    plane_peer = [z * PLANE + lax.rem(j + d, PLANE) for d in range(PLANE)]
    z_peer = [lax.rem(z + d, PLANES) * PLANE + j for d in range(PLANES)]

    @pl.when(b > 0)
    def _():
        greet(b - 1)

    @pl.when(b < PLANE * PLANES - 1)
    def _():
        greet(b + 1)

    for d in range(1, PLANE):
        greet(plane_peer[d])
    for d in range(1, PLANES):
        greet(z_peer[d])

    va[96] = jnp.zeros((COLS, LEAF), jnp.bfloat16)
    vb[96] = jnp.zeros((COLS, LEAF), jnp.bfloat16)
    dl[96] = jnp.zeros((COLS, 128), jnp.bfloat16)
    dr[96] = jnp.zeros((COLS, 128), jnp.bfloat16)

    def remote(src, dst, send, recv, target):
        return pltpu.make_async_remote_copy(
            src_ref=src, dst_ref=dst, send_sem=send, recv_sem=recv,
            device_id=(target, col), device_id_type=pl.DeviceIdType.MESH,
        )

    def halo_sends(m, mine, to_right, to_left, send, recv):
        return (
            remote(mine, to_right, send.at[m, 0], recv.at[m, 0], b + 1),
            remote(mine, to_left, send.at[m, 1], recv.at[m, 1], b - 1),
        )

    has_right = b < PLANE * PLANES - 1
    has_left = b > 0

    def halo_start(copies):
        @pl.when(has_right)
        def _():
            copies[0].start()

        @pl.when(has_left)
        def _():
            copies[1].start()

    def near_copies(copies, early):
        @pl.when(has_right if early else j < PLANE - 1)
        def _():
            copies[0].start()

        @pl.when(has_left if early else j > 0)
        def _():
            copies[1].start()

    def late_copies(copies):
        @pl.when(jnp.logical_and(has_right, j == PLANE - 1))
        def _():
            copies[0].start()

        @pl.when(jnp.logical_and(has_left, j == 0))
        def _():
            copies[1].start()

    def halo_recv(copies):
        @pl.when(has_left)
        def _():
            copies[0].wait_recv()

        @pl.when(has_right)
        def _():
            copies[1].wait_recv()

    def halo_sent(copies):
        @pl.when(has_right)
        def _():
            copies[0].wait_send()

        @pl.when(has_left)
        def _():
            copies[1].wait_send()

    def halves(pair):
        turned = pltpu.roll(pair, 64, 1)
        none = jnp.zeros_like(pair)
        return (
            jnp.where(left, pair, none).astype(jnp.bfloat16),
            jnp.where(left, none, turned).astype(jnp.bfloat16),
            jnp.where(left, turned, none).astype(jnp.bfloat16),
            jnp.where(left, none, pair).astype(jnp.bfloat16),
        )

    def put_halves(leaf, pair):
        al, ar, bl, br = halves(pair)
        dl[leaf] = al
        dr[leaf] = ar
        dl[leaf + 1] = bl
        dr[leaf + 1] = br

    def coef_pair(m, source, cp, p):
        lhs = source[pl.ds(LEAF_DEV + 2 * p, 2)].reshape(2 * COLS, LEAF)
        rhs = basis_w[m, pl.ds(2 * p, 2)].reshape(128, LEAF)
        both = dot_nt(lhs, rhs)
        got = jnp.where(left, both[:COLS], both[COLS:])
        cp[:, pl.ds(pl.multiple_of(LEAF_DEV * RANK + p * 128, 128), 128)] = got.astype(jnp.bfloat16)
        put_halves(LEAF_DEV + 2 * p, got)

    def masked_half(both, parity):
        keep = jnp.logical_xor(left, parity == 1)
        return jnp.where(keep, both, jnp.zeros_like(both)).astype(jnp.bfloat16)

    def live_or_zero(q, count, leaf):
        dead = lax.shift_right_arithmetic(q - count, 31) + 1
        return (leaf - first_leaf) + dead * (96 - (leaf - first_leaf))

    def far_rows(i):
        count = far_count[i]

        def spot(q):
            return live_or_zero(q, count, far_ids[q, i])

        return jnp.concatenate([dl[spot(2 * t)] + dr[spot(2 * t + 1)] for t in range(4)], axis=1)

    def near_rest(m, source, i):
        total = near_acc[:, pl.ds(pl.multiple_of(i * LEAF, LEAF), LEAF)]
        count = near_count[i]
        for q in range(1, 4):
            piece = source[live_or_zero(q, count, near_ids[q, i])]
            total = total + dot_nt(piece, near_w[m, i, q])
        return total

    def far_terms(m, p):
        pair = field[:, pl.ds(pl.multiple_of(p * 128, 128), 128)]
        none = jnp.zeros_like(pair)
        lhs = jnp.concatenate([jnp.where(left, pair, none), jnp.where(left, none, pair)], axis=0).astype(jnp.bfloat16)
        rhs = basis_w[m, pl.ds(2 * p, 2)].reshape(128, LEAF)
        both = dot_nn(lhs, rhs)
        return both[:COLS], both[COLS:]

    def chunk_copies(m, g):
        source = va if m == 0 else vb
        return halo_sends(
            m,
            source.at[pl.ds(LEAF_DEV + g * STEP, STEP)],
            source.at[pl.ds(g * STEP, STEP)],
            source.at[pl.ds(2 * LEAF_DEV + g * STEP, STEP)],
            v_send, v_recv,
        )

    def start_chunk(g):
        halo_start(chunk_copies(1, g))

    for m in range(2):
        source = va if m == 0 else vb
        cp = cpa if m == 0 else cpb
        if m == 0:
            load_v.wait()
            load_basis[0].wait()

            def coef_body(p, carry):
                coef_pair(0, va, cpa, p)
                return carry

            lax.fori_loop(0, LEAF_DEV // 2, coef_body, 0, unroll=8)
        load_trans[m].wait()
        box = dot_nt(cp[:, pl.ds(LEAF_DEV * RANK, LEAF_DEV * RANK)], trans_w[m])
        l0[m, 3 + j] = masked_half(jnp.concatenate([box, box], axis=1), core)
        if m == 0:
            last = PLANE * PLANES - 1
            pl.semaphore_wait(barrier, 14 + (b + last) // (last + 1) + (2 * last - b) // (last + 1))
        plane = []
        for d in range(1, PLANE):
            copy = remote(l0.at[m, 3 + j], l0.at[m, 3 + j], p_send.at[m, d], p_recv.at[m, d], plane_peer[d])
            copy.start()
            plane.append(copy)
        flat = LEAF_DEV * RANK
        coef_halo = halo_sends(
            m, cp.at[:, pl.ds(flat, flat)], cp.at[:, pl.ds(0, flat)], cp.at[:, pl.ds(2 * flat, flat)], c_send, c_recv
        )
        halo_start(coef_halo)
        vec_halo = halo_sends(
            m, source.at[own], source.at[pl.ds(0, LEAF_DEV)], source.at[pl.ds(2 * LEAF_DEV, LEAF_DEV)], v_send, v_recv
        )
        if m == 0:
            for g in range(CHUNKS):
                near_copies(chunk_copies(0, g), g < EARLY)
            start_rest(0)
        else:
            for g in range(CHUNKS - HELD, CHUNKS):
                start_chunk(g)

        if m == 0:
            for copy in load_small:
                copy.wait()
            load_ut.wait()
            load_uc.wait()
            for mm in range(2):
                for h in range(5):
                    blocks = []
                    for q in range(4):
                        one = up_c[mm, h, :, q * RANK:(q + 1) * RANK]
                        blocks += [one, one]
                    cc[mm, h] = jnp.concatenate(blocks, axis=1)
                chain = None
                for h in range(4):
                    half = jnp.where(lax.rem(b // (1 << h), 2) == 0, up_t[mm, h, :, :RANK], up_t[mm, h, :, RANK:])
                    chain = half if chain is None else dot_nn(half, chain).astype(jnp.bfloat16)
                    down_w[mm, h] = chain

        for copy in load_near[m][:2]:
            copy.wait()

        def own_body(i, carry):
            near_acc[:, pl.ds(pl.multiple_of(i * LEAF, LEAF), LEAF)] = dot_nt(source[LEAF_DEV + i], near_w[m, i, 0])
            return carry

        lax.fori_loop(0, LEAF_DEV, own_body, 0, unroll=16)

        for copy in plane:
            copy.wait_recv()

        def lift(pairs, h):
            weight = up_t[m, h]
            return dot_nt(pairs, jnp.concatenate([weight, weight], axis=0))

        pairs = jnp.concatenate([l0[m, 3 + 2 * i] + l0[m, 4 + 2 * i] for i in range(4)], axis=0)
        lifted = lift(pairs, 0)
        n1 = [masked_half(lifted[i * COLS:(i + 1) * COLS], i % 2) for i in range(4)]
        for i in range(4):
            l1[m, 3 + i] = n1[i]
        lifted = lift(jnp.concatenate([n1[0] + n1[1], n1[2] + n1[3]], axis=0), 1)
        n2 = [masked_half(lifted[i * COLS:(i + 1) * COLS], i % 2) for i in range(2)]
        for i in range(2):
            l2[m, 4 + i] = n2[i]
        l3[m, z] = masked_half(lift(n2[0] + n2[1], 2), lax.rem(z, 2))

        across = [None]
        for d in range(1, PLANES):
            across.append(remote(l3.at[m, z], l3.at[m, z], z_send.at[m, d], z_recv.at[m, d], z_peer[d]))
        for d in (4, 3, 5, 2, 6, 1, 7):
            across[d].start()
        across = across[1:]
        up_one = b + PLANE
        down_one = b - PLANE
        up_two = b + 2 * PLANE
        down_two = b - 2 * PLANE

        def edge(k, src, dst, target):
            return remote(src, dst, e_send.at[m, k], e_recv.at[m, k], target)

        ups = [
            edge(0, l2.at[m, pl.ds(4, 2)], l2.at[m, pl.ds(2, 2)], up_one),
            edge(1, l1.at[m, pl.ds(4, 3)], l1.at[m, pl.ds(0, 3)], up_one),
            edge(2, l0.at[m, pl.ds(8, 3)], l0.at[m, pl.ds(0, 3)], up_one),
        ]
        downs = [
            edge(3, l2.at[m, pl.ds(4, 2)], l2.at[m, pl.ds(6, 2)], down_one),
            edge(4, l1.at[m, pl.ds(3, 3)], l1.at[m, pl.ds(7, 3)], down_one),
            edge(5, l0.at[m, pl.ds(3, 3)], l0.at[m, pl.ds(11, 3)], down_one),
        ]
        up2 = edge(6, l2.at[m, pl.ds(4, 2)], l2.at[m, pl.ds(0, 2)], up_two)
        down2 = edge(7, l2.at[m, pl.ds(4, 2)], l2.at[m, pl.ds(8, 2)], down_two)

        @pl.when(z + 1 < PLANES)
        def _():
            for copy in ups:
                copy.start()

        @pl.when(z > 0)
        def _():
            for copy in downs:
                copy.start()

        @pl.when(z + 2 < PLANES)
        def _():
            up2.start()

        @pl.when(z > 1)
        def _():
            down2.start()

        if m == 0:
            for g in range(EARLY, CHUNKS):
                late_copies(chunk_copies(0, g))
            start_first(1)
            start_rest(1)
        halo_recv(coef_halo)

        def dup_body(p, carry):
            for spot in (p, p + LEAF_DEV):
                pair = cp[:, pl.ds(pl.multiple_of(spot * 128, 128), 128)].astype(jnp.float32)
                put_halves(2 * spot, pair)
            return carry

        lax.fori_loop(0, LEAF_DEV // 2, dup_body, 0, unroll=8)
        load_coup[m].wait()

        def coup_body(p, carry):
            lhs = jnp.concatenate([far_rows(2 * p), far_rows(2 * p + 1)], axis=0)
            rhs = coup_w[m, pl.ds(2 * p, 2)].reshape(128, 512)
            both = dot_nt(lhs, rhs)
            field[:, pl.ds(pl.multiple_of(p * 128, 128), 128)] = jnp.where(left, both[:COLS], both[COLS:])
            return carry

        lax.fori_loop(0, LEAF_DEV // 2, coup_body, 0, unroll=8)

        for copy in load_near[m][2:]:
            copy.wait()
        halo_recv(vec_halo)

        def near_body(i, carry):
            near_acc[:, pl.ds(pl.multiple_of(i * LEAF, LEAF), LEAF)] = near_rest(m, source, i)
            return carry

        lax.fori_loop(0, AHEAD * STEP if m == 0 else LEAF_DEV, near_body, 0, unroll=16 if m else 8)

        @pl.when(z + 1 < PLANES)
        def _():
            for copy in downs:
                copy.wait_recv()

        @pl.when(z > 0)
        def _():
            for copy in ups:
                copy.wait_recv()

        @pl.when(z + 2 < PLANES)
        def _():
            down2.wait_recv()

        @pl.when(z > 1)
        def _():
            up2.wait_recv()

        def node(h, o):
            if h == 0:
                return l0[m, 3 + j + o]
            if h == 1:
                return l1[m, 3 + x + o]
            if h == 2:
                return l2[m, 4 + x // 2 + o]
            if h == 3:
                return l3[m, lax.rem(z + o + PLANES, PLANES)]
            return l4[lax.rem(z // 2 + o + 4, 4)]

        def coupled(h):
            n = b // (1 << h)
            blocks = []
            for q, o in enumerate(OFFSETS):
                there = jnp.logical_and(n + o >= 0, n + o < (64 >> h))
                live = jnp.full((COLS, 128), far_mask[h, q, n].astype(jnp.float32)).astype(jnp.bfloat16)
                blocks.append(jnp.where(there, node(h, o), jnp.zeros((COLS, 128), jnp.bfloat16)) * live)
            return dot_nt(jnp.concatenate(blocks, axis=1), cc[m, h])

        def brought(h, term):
            return dot_nn(term.astype(jnp.bfloat16), down_w[m, h - 1])

        descent = coupled(0) + brought(1, coupled(1)) + brought(2, coupled(2))

        for copy in across:
            copy.wait_recv()

        descent = descent + brought(3, coupled(3))
        pairs = jnp.concatenate([l3[m, 2 * i] + l3[m, 2 * i + 1] for i in range(4)], axis=0)
        lifted = lift(pairs, 3)
        for i in range(4):
            l4[i] = masked_half(lifted[i * COLS:(i + 1) * COLS], 0)
        descent = descent + brought(4, coupled(4))
        parent = descent.astype(jnp.bfloat16)
        field[...] += dot_nn(parent, trans_w[m])

        if m == 0:
            load_basis[1].wait()

            def coef_chunk(g):
                for k in range(STEP // 2):
                    coef_pair(1, vb, cpb, g * (STEP // 2) + k)

            def join(g, near):
                for k in range(STEP // 2):
                    p = g * (STEP // 2) + k
                    far = far_terms(0, p)
                    for s in range(2):
                        i = 2 * p + s
                        total = near_rest(0, va, i) if near else near_acc[:, pl.ds(pl.multiple_of(i * LEAF, LEAF), LEAF)]
                        vb[LEAF_DEV + i] = (total + far[s]).astype(jnp.bfloat16)

            def ready_body(g, carry):
                coef_chunk(g - (g + CHUNKS - 1) // CHUNKS)
                join(g, False)

                @pl.when(g > 0)
                def _():
                    start_chunk(g - 1)

                return carry

            def join_body(g, carry):
                coef_chunk(AHEAD + g - 1)
                join(AHEAD + g, True)

                @pl.when(AHEAD + g <= CHUNKS - HELD)
                def _():
                    start_chunk(AHEAD + g - 1)

                return carry

            lax.fori_loop(0, AHEAD, ready_body, 0)
            lax.fori_loop(0, CHUNKS - AHEAD, join_body, 0)
            coef_chunk(CHUNKS - 1)
        else:

            def final_body(p, carry):
                far = far_terms(1, p)
                total = near_acc[:, pl.ds(pl.multiple_of(p * 512, 512), 512)]
                for s in range(2):
                    where_to = pl.ds(pl.multiple_of(p * 512 + s * LEAF, LEAF), LEAF)
                    out[:, where_to] = (total[:, s * LEAF:(s + 1) * LEAF] + far[s]).astype(jnp.bfloat16)
                return carry

            lax.fori_loop(0, LEAF_DEV // 2, final_body, 0, unroll=8)

        for copy in plane + across:
            copy.wait_send()
        halo_sent(coef_halo)
        halo_sent(vec_halo)

        @pl.when(z + 1 < PLANES)
        def _():
            for copy in ups:
                copy.wait_send()

        @pl.when(z > 0)
        def _():
            for copy in downs:
                copy.wait_send()

        @pl.when(z + 2 < PLANES)
        def _():
            up2.wait_send()

        @pl.when(z > 1)
        def _():
            down2.wait_send()


def shards(
    vectors, basis, leaf_transfer, upper_transfer, upper_coupling, leaf_coupling, near_blocks,
    far_mask, far_ids, far_count, near_ids, near_count,
):
    smem = pltpu.SMEM
    i32 = jnp.int32
    hbm = pl.BlockSpec(memory_space=pltpu.HBM)
    bf = jnp.bfloat16
    f32 = jnp.float32
    dma = pltpu.SemaphoreType.DMA
    return pl.pallas_call(
        kernel,
        out_shape=jax.ShapeDtypeStruct((COLS, LEAF_DEV * LEAF), bf),
        in_specs=[hbm] * 12,
        out_specs=pl.BlockSpec(memory_space=pltpu.VMEM),
        scratch_shapes=[
            smem((5, 4, 64), i32), smem((8, LEAF_DEV), i32), smem((LEAF_DEV,), i32), smem((4, LEAF_DEV), i32), smem((LEAF_DEV,), i32),
            pltpu.VMEM((2, LEAF_DEV, 4, LEAF, LEAF), bf),
            pltpu.VMEM((2, LEAF_DEV, RANK, 512), bf),
            pltpu.VMEM((2, LEAF_DEV, RANK, LEAF), bf),
            pltpu.VMEM((2, RANK, LEAF_DEV * RANK), bf),
            pltpu.VMEM((2, 4, RANK, 128), bf),
            pltpu.VMEM((2, 5, RANK, 256), bf),
            pltpu.VMEM((97, COLS, LEAF), bf),
            pltpu.VMEM((97, COLS, LEAF), bf),
            pltpu.VMEM((COLS, 96 * RANK), bf),
            pltpu.VMEM((COLS, 96 * RANK), bf),
            pltpu.VMEM((97, COLS, 128), bf),
            pltpu.VMEM((97, COLS, 128), bf),
            pltpu.VMEM((COLS, LEAF_DEV * LEAF), f32),
            pltpu.VMEM((COLS, LEAF_DEV * RANK), f32),
            pltpu.VMEM((2, 14, COLS, 128), bf),
            pltpu.VMEM((2, 10, COLS, 128), bf),
            pltpu.VMEM((2, 10, COLS, 128), bf),
            pltpu.VMEM((2, 8, COLS, 128), bf),
            pltpu.VMEM((4, COLS, 128), bf),
            pltpu.VMEM((2, 5, RANK, 512), bf),
            pltpu.VMEM((2, 4, RANK, RANK), bf),
            dma((2, CHUNKS)), dma((9,)), dma((5,)),
            dma((2, 2)), dma((2, 2)), dma((2, 2)), dma((2, 2)),
            dma((2, 8)), dma((2, 8)), dma((2, 8)), dma((2, 8)), dma((2, 8)), dma((2, 8)),
        ],
        compiler_params=pltpu.CompilerParams(
            collective_id=0, has_side_effects=True, vmem_limit_bytes=50 << 20
        ),
        name="product",
    )(
        *(
            pltpu.with_memory_space_constraint(array, pltpu.HBM)
            for array in (
                jnp.transpose(far_mask, (0, 2, 1)), far_ids.T, far_count, near_ids.T, near_count,
                vectors, basis, leaf_transfer, upper_transfer, upper_coupling, leaf_coupling, near_blocks,
            )
        )
    )


def solution(mesh):
    return jax.shard_map(
        shards,
        mesh=mesh,
        in_specs=(
            P("col", "branch"),
            P(None, "branch", None, None),
            P(None, None, "branch"),
            P(),
            P(),
            P(None, "branch", None, None),
            P(None, "branch", None, None, None),
            P(),
            P("branch", None),
            P("branch"),
            P("branch", None),
            P("branch"),
        ),
        out_specs=P("col", "branch"),
        check_vma=False,
    )
```
